256 devices in a mesh: layer: 16 (over y, x_hi, core), feat: 16 (over z, x_lo).
Axes of the slice: x: 4 (x_hi: 2, x_lo: 2; x = x_hi * 2 + x_lo), y: 4, z: 8, core: 2. Of those that a mesh axis runs over, the one named last changes fastest.
Arguments:
- residual_in: bfloat16 [16, 256, 4096], P('layer', None, 'feat'), may hold values from -6 to 6
- mlp_out: bfloat16 [16, 256, 4096], P('layer', None, 'feat'), may hold values from -6 to 6
- encoder: bfloat16 [16, 4096, 2048], P('layer', None, 'feat'), may hold values from -0.09375 to 0.09375
- encoder_bias: float32 [16, 2048], P('layer', 'feat'), may hold values from -3 to 3
- decoder: bfloat16 [16, 9, 2048, 4096], P('layer', None, 'feat'), may hold values from -0.046875 to 0.046875
- decoder_bias: float32 [16, 4096], P('layer'), may hold values from -3 to 3
Outputs:
- recon_error: bfloat16 [16, 256, 4096], P('layer', None, 'feat')
- pre_grad: float32 [16, 256, 2048], P('layer', None, 'feat')
The draws below stay inside these ranges and needn't reach their ends.
All inputs are finite; a program needn't handle non-finite values.
Results may differ from the reference program's by a relative error of at most 0.0035.
Values may be sent and summed in bfloat16 or wider, within the bound.
A program may use at most 128 MiB of HBM per device.

```python
import jax
import jax.numpy as jnp

D = 4096
TOK = 256
LAYERS = 16
SLOTS = 9
FEAT = 2048


def shard_levels(stream_key, dims, shards, least, high):
    gain = 1.0
    for position, blocks in shards:
        steps = jax.random.uniform(jax.random.fold_in(jax.random.fold_in(stream_key, 6), position), (blocks,), jnp.float32, least / len(shards), high / len(shards))
        gain = gain * jnp.repeat(jnp.exp(steps), dims[position] // blocks).reshape((-1,) + (1,) * (len(dims) - 1 - position))
    return gain


def scatter_about(rng, dims, width, bound, pieces=(), held_as=jnp.bfloat16):
    array = jax.random.normal(rng, dims, jnp.float32) * width
    if len(pieces) > 0:
        array = shard_levels(rng, dims, pieces, -0.22, 0.18) * array
    return jnp.clip(array, min=-bound, max=bound).astype(held_as)


def setup_inputs(seed: int = 0) -> dict:
    key_list = jax.random.split(jax.random.key(seed), 7)
    return {
        "residual_in": scatter_about(key_list[0], (LAYERS, TOK, D), 1.0, 6.0, ((0, 16), (2, 16))),
        "mlp_out": scatter_about(key_list[1], (LAYERS, TOK, D), 1.0, 6.0, ((0, 16), (2, 16))),
        "encoder": scatter_about(key_list[2], (LAYERS, D, FEAT), D ** -0.5, 0.09375, ((0, 16), (2, 16))),
        "encoder_bias": scatter_about(key_list[3], (LAYERS, FEAT), 0.5, 3.0, ((0, 16), (1, 16)), jnp.float32),
        "decoder": scatter_about(key_list[4], (LAYERS, SLOTS, FEAT, D), (FEAT * LAYERS // 2) ** -0.5, 0.046875, ((0, 16), (2, 16))),
        "decoder_bias": scatter_about(key_list[5], (LAYERS, D), 0.5, 3.0, ((0, 16),), jnp.float32),
    }


def decoder_block(decoder, source, target):
    half_layers = LAYERS // 2
    if source <= min(target, half_layers - 1):
        return decoder[target, source]
    mirror_row = LAYERS - 1 - target
    return decoder[mirror_row, source - half_layers + mirror_row + 1]


def reference(residual_in, mlp_out, encoder, encoder_bias, decoder, decoder_bias):
    codes = []
    for layer_idx in range(LAYERS):
        value = jnp.dot(residual_in[layer_idx], encoder[layer_idx], preferred_element_type=jnp.float32) + encoder_bias[layer_idx][None, :]
        codes.append(jnp.maximum(value, 0.0).astype(jnp.bfloat16))
    errors = []
    for target in range(LAYERS):
        recon = jnp.zeros((TOK, D), jnp.float32) + decoder_bias[target][None, :]
        for source in range(target + 1):
            recon = recon + jnp.dot(codes[source], decoder_block(decoder, source, target), preferred_element_type=jnp.float32)
        errors.append((recon - mlp_out[target].astype(jnp.float32)).astype(jnp.bfloat16))
    grads = []
    for source in range(LAYERS):
        back = jnp.zeros((TOK, FEAT), jnp.float32)
        for target in range(source, LAYERS):
            back = back + jnp.dot(errors[target], decoder_block(decoder, source, target).T, preferred_element_type=jnp.float32)
        grads.append(back)
    return jnp.stack(errors), jnp.stack(grads)
```

```python
import functools

import jax
import jax.numpy as jnp
from jax import lax
from jax.experimental import pallas as pl
from jax.experimental.pallas import tpu as pltpu
from jax.sharding import Mesh
from jax.sharding import PartitionSpec as P

MESH = pl.DeviceIdType.MESH
ZS = 8
FEAT = ("z", "xl")


def around(v, step):
    return lax.rem(v + step + ZS, ZS)


def remote(src, dst, send_sem, recv_sem, **where):
    return pltpu.make_async_remote_copy(
        src_ref=src, dst_ref=dst, send_sem=send_sem, recv_sem=recv_sem, device_id=where, device_id_type=MESH
    )


class Gather:
    def __init__(self, buf, send, recv, z, xl):
        self.buf, self.send, self.recv, self.z, self.xl = buf, send, recv, z, xl
        self.own = 2 * z + xl
        self.other = 2 * z + 1 - xl
        self.up, self.down = around(z, 1), around(z, -1)
        self.sent = []

    def copy(self, way, block):
        where = ({"z": self.up}, {"z": self.down}, {"xl": 1 - self.xl})[way]
        at = self.buf.at[block]
        return remote(at, at, self.send.at[way, block], self.recv.at[block], **where)

    def push(self, way, block):
        self.copy(way, block).start()

    def arrive(self, block):
        self.copy(0, block).wait_recv()

    def begin(self):
        for way in (2, 0, 1):
            self.push(way, self.own)

    def relay(self):
        self.arrive(self.other)
        for way in (0, 1):
            self.push(way, self.other)

    def blocks(self, d):
        out = []
        for col in (0, 1):
            for way in (0, 1):
                if d < 4 or way == col:
                    out.append((way, col, 2 * around(self.z, d if way else -d) + col))
        return out

    def step(self, d):
        for way, col, block in self.blocks(d):
            self.arrive(block)
            if d < 3 or (d == 3 and way == col):
                self.push(way, block)

    def drain(self):
        for way in (0, 1, 2):
            self.copy(way, self.own).wait_send()
        for way in (0, 1):
            self.copy(way, self.other).wait_send()
        for d in (1, 2, 3):
            for way, col, block in self.blocks(d):
                if d < 3 or way == col:
                    self.copy(way, block).wait_send()


def greet(z, xl, me, rows):
    barrier = pltpu.get_barrier_semaphore()
    peers = [{"z": around(z, 1)}, {"z": around(z, -1)}, {"xl": 1 - xl}]
    if rows:
        peers += [{"layer": lax.rem(me + k, rows)} for k in range(1, rows)]
    for peer in peers:
        pl.semaphore_signal(barrier, inc=1, device_id=peer, device_id_type=MESH)
    pl.semaphore_wait(barrier, len(peers))


def encode_kernel(res_ref, enc_ref, bias_ref, codes_ref, buf, acc, send, recv, in_sem):
    z, xl = lax.axis_index("z"), lax.axis_index("xl")
    gather = Gather(buf, send, recv, z, xl)
    load = pltpu.make_async_copy(res_ref, buf.at[gather.own], in_sem)
    load.start()
    greet(z, xl, None, 0)
    load.wait()
    gather.begin()
    width = res_ref.shape[1]

    def add(block):
        rows = pl.ds(pl.multiple_of(block * width, width), width)
        acc[...] += jnp.dot(buf[block], enc_ref[rows, :], preferred_element_type=jnp.float32)

    acc[...] = jnp.zeros_like(acc) + bias_ref[...]
    add(gather.own)
    gather.relay()
    add(gather.other)
    for d in (1, 2, 3, 4):
        gather.step(d)
        for _, _, block in gather.blocks(d):
            add(block)
    codes_ref[...] = jnp.maximum(acc[...], 0.0).astype(codes_ref.dtype)
    gather.drain()


def needs(row, source, layers):
    half = layers // 2
    low = source < half
    wanted = (low & (row >= source)) | (jnp.logical_not(low) & (row <= layers - 1 - source))
    return wanted, jnp.where(low, source, source - (half - 1) + row)


def step_kernel(
    layers,
    codes_ref,
    dec_ref,
    bias_ref,
    mlp_ref,
    err_ref,
    grad_ref,
    weights,
    code_slots,
    rows_in,
    part,
    ring_out,
    ring_in,
    cross_out,
    cross_in,
    mirror_out,
    mirror_in,
    errors,
    terms_out,
    terms_in,
    w_sem,
    code_send,
    code_recv,
    ring_send,
    ring_recv,
    cross_send,
    cross_recv,
    mirror_send,
    mirror_recv,
    back_send,
    gather_send,
    gather_recv,
    term_send,
    term_recv,
):
    half = layers // 2
    me, z, xl = lax.axis_index("layer"), lax.axis_index("z"), lax.axis_index("xl")
    slots, tokens, feats = code_slots.shape
    width = part.shape[3]
    heavy = me < half
    own_slots = jnp.where(heavy, me + 1, half)
    all_slots = jnp.where(heavy, slots, half)
    mirror = layers - 1 - me
    up, down = around(z, 1), around(z, -1)
    mine = 2 * z + xl

    load = pltpu.make_async_copy(dec_ref, weights, w_sem)
    load.start()
    greet(z, xl, me, layers)

    def code_copy(k):
        row = lax.rem(me + k, layers)
        wanted, slot = needs(row, me, layers)
        slot = jnp.where(wanted, slot, 0)
        return wanted, remote(codes_ref, code_slots.at[slot], code_send.at[k], code_recv.at[slot], layer=row)

    for k in range(1, layers):
        wanted, copy = code_copy(k)
        pl.when(wanted)(copy.start)

    @pl.when(heavy)
    def _():
        code_slots[me] = codes_ref[...]

    @pl.when(jnp.logical_not(heavy))
    def _():
        code_slots[slots - 1] = jnp.zeros((tokens, feats), code_slots.dtype)

    for j in range(slots):
        copy = remote(codes_ref, code_slots.at[j], code_send.at[0], code_recv.at[j], layer=mirror)
        pl.when((j < all_slots) & (jnp.logical_not(heavy) | (me != j)))(copy.wait_recv)

    for j in range(slots):
        cols = pl.ds(j * feats, feats)
        block = code_slots[j]
        own = j < own_slots
        rows_in[0, :, cols] = jnp.where(own, block, jnp.zeros_like(block))
        rows_in[1, :, cols] = jnp.where(own, jnp.zeros_like(block), block)
    load.wait()

    def decode(a, blocks):
        for block in blocks:
            cols = pl.ds(pl.multiple_of(block * width, width), width)
            part[a, block] = jnp.dot(rows_in[a], weights[:, cols], preferred_element_type=jnp.float32)

    def target(way, d):
        return around(z, -d if way else d)

    def ring_copy(a, way, j, col):
        return remote(
            ring_out.at[a, way, j, col],
            ring_in.at[a, way, j, col],
            ring_send.at[a, way, j, col],
            ring_recv.at[a, way, j, col],
            z=down if way else up,
        )

    def ring_pieces(j):
        return [(way, col) for col in (0, 1) for way in (0, 1) if j > 0 or way == col]

    def ring_decode(a, j):
        decode(a, [2 * target(way, 4 - j) + col for way, col in ring_pieces(j)])

    def ring_step(a, j):
        before = ring_pieces(j - 1) if j else []
        for way, col in ring_pieces(j):
            value = part[a, 2 * target(way, 4 - j) + col]
            if (way, col) in before:
                ring_copy(a, way, j - 1, col).wait_recv()
                value = value + ring_in[a, way, j - 1, col].astype(jnp.float32)
            ring_out[a, way, j, col] = value.astype(jnp.bfloat16)
            ring_copy(a, way, j, col).start()

    def cross_copy(a):
        return remote(cross_out.at[a], cross_in.at[a], cross_send.at[a], cross_recv.at[a], xl=1 - xl)

    def ring_end(a):
        for col in (0, 1):
            for way in (0, 1):
                ring_copy(a, way, 3, col).wait_recv()

        def total(col):
            both = ring_in[a, 0, 3, col].astype(jnp.float32) + ring_in[a, 1, 3, col].astype(jnp.float32)
            return part[a, 2 * z + col] + both

        cross_out[a] = total(1 - xl).astype(jnp.bfloat16)
        cross_copy(a).start()
        part[a, mine] = total(xl)

    def ring_sum(a):
        cross_copy(a).wait_recv()
        return part[a, mine] + cross_in[a].astype(jnp.float32)

    def mirror_copy():
        return remote(mirror_out, mirror_in, mirror_send, mirror_recv, layer=mirror)

    on_heavy = pl.when(heavy)
    on_light = pl.when(jnp.logical_not(heavy))
    for j in range(4):
        on_heavy(lambda j=j: ring_decode(1, j))
        if j == 0:
            on_heavy(lambda: ring_step(1, 0))
        ring_decode(0, j)
        if j > 0:
            on_heavy(lambda j=j: ring_step(1, j))
        ring_step(0, j)
    on_heavy(lambda: decode(1, [2 * z, 2 * z + 1]))
    decode(0, [2 * z, 2 * z + 1])

    on_heavy(lambda: ring_end(1))
    ring_end(0)

    @on_heavy
    def _():
        mirror_out[...] = ring_sum(1).astype(jnp.bfloat16)
        mirror_copy().start()

    share = ring_sum(0) + bias_ref[pl.ds(mine, 1), :] - mlp_ref[...].astype(jnp.float32)
    part[0, mine] = share

    @on_light
    def _():
        mirror_copy().wait_recv()
        part[0, mine] = part[0, mine] + mirror_in[...].astype(jnp.float32)

    error = part[0, mine].astype(jnp.bfloat16)
    err_ref[...] = error
    errors[0, mine] = error

    gathers = [Gather(errors.at[a], gather_send.at[a], gather_recv.at[a], z, xl) for a in (0, 1)]

    def back_copy():
        return remote(errors.at[0, mine], errors.at[1, mine], back_send, back_recv_sem(), layer=mirror)

    def back_recv_sem():
        return gather_recv.at[1, mine]

    on_light(lambda: back_copy().start())
    first, second = gathers
    first.begin()
    first.relay()
    first.step(1)
    first.step(2)

    @on_heavy
    def _():
        back_copy().wait_recv()
        second.begin()

    first.step(3)
    on_heavy(second.relay)
    first.step(4)
    on_heavy(lambda: second.step(1))

    grad_ref[...] = jnp.zeros_like(grad_ref)

    def term_copy(j):
        source = jnp.where(j < own_slots, j, j + (half - 1) - me)
        return source, remote(
            terms_out.at[j], terms_in.at[me], term_send.at[j], term_recv.at[me], layer=source
        )

    def backward(a):
        def one(j, carry):
            rows = pl.ds(pl.multiple_of(j * feats, feats), feats)
            total = jnp.zeros((tokens, feats), jnp.float32)
            for block in range(2 * ZS):
                total = total + lax.dot_general(
                    errors[a, block],
                    weights[rows, block * width : (block + 1) * width],
                    (((1,), (1,)), ((), ())),
                    preferred_element_type=jnp.float32,
                )
            source, copy = term_copy(j)

            @pl.when(source == me)
            def _():
                grad_ref[...] = total

            @pl.when(source != me)
            def _():
                terms_out[j] = total.astype(terms_out.dtype)
                copy.start()

            return carry

        return one

    lax.fori_loop(0, own_slots, backward(0), 0)

    @on_heavy
    def _():
        second.step(2)
        second.step(3)
        second.step(4)
        lax.fori_loop(own_slots, slots, backward(1), 0)

    def collect(row, carry):
        wanted, _ = needs(row, me, layers)

        @pl.when(wanted & (row != me))
        def _():
            remote(terms_out.at[0], terms_in.at[row], term_send.at[0], term_recv.at[row], layer=mirror).wait_recv()
            grad_ref[...] += terms_in[row].astype(jnp.float32)

        return carry

    lax.fori_loop(0, layers, collect, 0)

    for k in range(1, layers):
        wanted, copy = code_copy(k)
        pl.when(wanted)(copy.wait_send)

    def drain_sums(a):
        for j in range(4):
            for way, col in ring_pieces(j):
                ring_copy(a, way, j, col).wait_send()
        cross_copy(a).wait_send()

    drain_sums(0)
    first.drain()
    on_light(lambda: back_copy().wait_send())

    @on_heavy
    def _():
        drain_sums(1)
        mirror_copy().wait_send()
        second.drain()

    def drain_terms(j, carry):
        source, copy = term_copy(j)
        pl.when(source != me)(copy.wait_send)
        return carry

    lax.fori_loop(0, all_slots, drain_terms, 0)


def shards(residual_in, mlp_out, encoder, encoder_bias, decoder, decoder_bias):
    layers = lax.axis_size("layer")
    tokens, width = residual_in.shape[1:]
    feats = encoder.shape[2]
    slots = decoder.shape[1]
    depth = decoder.shape[3]
    blocks = 2 * ZS
    bf16, f32 = jnp.bfloat16, jnp.float32
    dma = pltpu.SemaphoreType.DMA
    vmem = pl.BlockSpec(memory_space=pltpu.VMEM)
    hbm = pl.BlockSpec(memory_space=pl.ANY)

    codes = pl.pallas_call(
        encode_kernel,
        out_shape=jax.ShapeDtypeStruct((tokens, feats), bf16),
        in_specs=[hbm, vmem, vmem],
        out_specs=vmem,
        scratch_shapes=[
            pltpu.VMEM((blocks, tokens, width), bf16),
            pltpu.VMEM((tokens, feats), f32),
            dma((3, blocks)),
            dma((blocks,)),
            dma,
        ],
        compiler_params=pltpu.CompilerParams(
            collective_id=0, has_side_effects=True, vmem_limit_bytes=16 << 20
        ),
        name="encode",
    )(residual_in[0], encoder[0], encoder_bias)

    error, grad = pl.pallas_call(
        functools.partial(step_kernel, layers),
        out_shape=(
            jax.ShapeDtypeStruct((tokens, width), bf16),
            jax.ShapeDtypeStruct((tokens, feats), f32),
        ),
        in_specs=[vmem, hbm, vmem, vmem],
        out_specs=(vmem, vmem),
        scratch_shapes=[
            pltpu.VMEM((slots * feats, depth), bf16),
            pltpu.VMEM((slots, tokens, feats), bf16),
            pltpu.VMEM((2, tokens, slots * feats), bf16),
            pltpu.VMEM((2, blocks, tokens, width), f32),
            pltpu.VMEM((2, 2, 4, 2, tokens, width), bf16),
            pltpu.VMEM((2, 2, 4, 2, tokens, width), bf16),
            pltpu.VMEM((2, tokens, width), bf16),
            pltpu.VMEM((2, tokens, width), bf16),
            pltpu.VMEM((tokens, width), bf16),
            pltpu.VMEM((tokens, width), bf16),
            pltpu.VMEM((2, blocks, tokens, width), bf16),
            pltpu.VMEM((slots, tokens, feats), bf16),
            pltpu.VMEM((layers, tokens, feats), bf16),
            dma,
            dma((layers,)),
            dma((slots,)),
            dma((2, 2, 4, 2)),
            dma((2, 2, 4, 2)),
            dma((2,)),
            dma((2,)),
            dma,
            dma,
            dma,
            dma((2, 3, blocks)),
            dma((2, blocks)),
            dma((slots,)),
            dma((layers,)),
        ],
        compiler_params=pltpu.CompilerParams(
            collective_id=1, has_side_effects=True, vmem_limit_bytes=56 << 20
        ),
        name="decode_backward",
    )(codes, decoder[0].reshape(slots * feats, depth), decoder_bias.reshape(blocks, width), mlp_out[0])
    return error[None], grad[None]


def solution(mesh):
    split = Mesh(mesh.devices.reshape(mesh.shape["layer"], ZS, 2), ("layer", "z", "xl"))
    placed = (
        P("layer", None, FEAT),
        P("layer", None, FEAT),
        P("layer", None, FEAT),
        P("layer", FEAT),
        P("layer", None, FEAT, None),
        P("layer", None),
    )
    return jax.shard_map(
        shards,
        mesh=split,
        in_specs=placed,
        out_specs=(P("layer", None, FEAT), P("layer", None, FEAT)),
        check_vma=False,
    )
```

```python
import functools

import jax
import jax.numpy as jnp
from jax import lax
from jax.experimental import pallas as pl
from jax.experimental.pallas import tpu as pltpu
from jax.sharding import Mesh
from jax.sharding import PartitionSpec as P

MESH = pl.DeviceIdType.MESH
ZS = 8
FEAT = ("z", "xl")
LEAD = 1


def around(v, step):
    return lax.rem(v + step + ZS, ZS)


def remote(src, dst, send_sem, recv_sem, **where):
    return pltpu.make_async_remote_copy(
        src_ref=src, dst_ref=dst, send_sem=send_sem, recv_sem=recv_sem, device_id=where, device_id_type=MESH
    )


class Gather:
    def __init__(self, buf, send, recv, z, xl, turn):
        self.buf, self.send, self.recv, self.z, self.xl, self.turn = buf, send, recv, z, xl, turn
        self.own = 2 * z + xl
        self.other = 2 * z + 1 - xl
        self.up, self.down = around(z, 1), around(z, -1)

    def copy(self, way, block):
        where = ({"z": self.up}, {"z": self.down}, {"xl": 1 - self.xl})[way]
        at = self.buf.at[block]
        return remote(at, at, self.send.at[way, block], self.recv.at[block], **where)

    def push(self, way, block):
        self.copy(way, block).start()

    def arrive(self, block):
        self.copy(0, block).wait_recv()

    def begin(self):
        for way in (2, 0, 1):
            self.push(way, self.own)

    def drain_own(self):
        for way in (0, 1, 2):
            self.copy(way, self.own).wait_send()


class Wide(Gather):
    def relay(self):
        self.arrive(self.other)
        for way in (0, 1):
            self.push(way, self.other)
        return [self.other]

    def blocks(self, d):
        out = []
        for col in (0, 1):
            for way in (0, 1):
                if d < 4 or way == col:
                    out.append((way, col, 2 * around(self.z, d if way else -d) + col))
        return out

    def step(self, d):
        for way, col, block in self.blocks(d):
            self.arrive(block)
            if d < 3 or (d == 3 and way == col):
                self.push(way, block)
        return [block for _, _, block in self.blocks(d)]

    def phases(self):
        return [self.relay] + [functools.partial(self.step, d) for d in (1, 2, 3, 4)]

    def drain(self):
        self.drain_own()
        for way in (0, 1):
            self.copy(way, self.other).wait_send()
        for d in (1, 2, 3):
            for way, col, block in self.blocks(d):
                if d < 3 or way == col:
                    self.copy(way, block).wait_send()


class Narrow(Gather):
    def blocks(self, d):
        if d == 4:
            return [(None, 2 * around(self.z, 4) + self.xl)]
        return [(way, 2 * around(self.z, d if way else -d) + self.xl) for way in (0, 1)]

    def crossed(self, d):
        places = [self.z] if d == 0 else [around(self.z, 4)] if d == 4 else [around(self.z, -d), around(self.z, d)]
        return [2 * place + 1 - self.xl for place in places]

    def step(self, d):
        out = []
        if d < 5:
            for way, block in self.blocks(d):
                self.arrive(block)
                if d < 3:
                    self.push(way, block)
                if d == 3:
                    pl.when(self.turn == way)(self.copy(way, block).start)
                self.push(2, block)
                out.append(block)
        for block in self.crossed(d - 1):
            self.arrive(block)
            out.append(block)
        return out

    def phases(self):
        return [functools.partial(self.step, d) for d in (1, 2, 3, 4, 5)]

    def drain(self):
        self.drain_own()
        for d in (1, 2, 3, 4):
            for way, block in self.blocks(d):
                if d < 3:
                    self.copy(way, block).wait_send()
                if d == 3:
                    pl.when(self.turn == way)(self.copy(way, block).wait_send)
                self.copy(2, block).wait_send()


def needs(row, source, layers):
    half = layers // 2
    low = source < half
    wanted = (low & (row >= source)) | (jnp.logical_not(low) & (row <= layers - 1 - source))
    return wanted, jnp.where(low, source, source - (half - 1) + row)


def step_kernel(
    layers,
    res_ref,
    mlp_ref,
    enc_ref,
    enc_bias_ref,
    dec_ref,
    dec_bias_ref,
    err_ref,
    grad_ref,
    residual,
    mlp,
    encoder,
    enc_bias,
    weights,
    dec_bias,
    preact,
    codes,
    code_slots,
    rows_in,
    part,
    ring_out,
    ring_in,
    cross_out,
    cross_in,
    hand_out,
    hand_in,
    mirror_out,
    mirror_in,
    errors,
    terms_out,
    terms_in,
    load_sem,
    res_send,
    res_recv,
    code_send,
    code_recv,
    ring_send,
    ring_recv,
    cross_send,
    cross_recv,
    hand_send,
    hand_recv,
    mirror_send,
    mirror_recv,
    back_send,
    gather_send,
    gather_recv,
    term_send,
    term_recv,
):
    half = layers // 2
    me, z, xl = lax.axis_index("layer"), lax.axis_index("z"), lax.axis_index("xl")
    _, slots, tokens, feats = code_slots.shape
    width = part.shape[4]
    bf16, f32 = jnp.bfloat16, jnp.float32
    heavy = me < half
    own_slots = jnp.where(heavy, me + 1, half)
    all_slots = jnp.where(heavy, slots, half)
    mirror = layers - 1 - me
    turn = lax.rem(me, 2)
    up, down = around(z, 1), around(z, -1)
    mine = 2 * z + xl
    on_heavy = pl.when(heavy)
    on_light = pl.when(jnp.logical_not(heavy))

    loads = [
        pltpu.make_async_copy(res_ref.at[pl.ds(h * tokens, tokens)], residual.at[h, mine], load_sem.at[h]) for h in (0, 1)
    ]
    loads += [
        pltpu.make_async_copy(enc_ref, encoder, load_sem.at[2]),
        pltpu.make_async_copy(enc_bias_ref, enc_bias, load_sem.at[3]),
        pltpu.make_async_copy(dec_ref, weights, load_sem.at[4]),
        pltpu.make_async_copy(mlp_ref, mlp, load_sem.at[5]),
        pltpu.make_async_copy(dec_bias_ref, dec_bias, load_sem.at[6]),
    ]
    for load in loads:
        load.start()

    barrier = pltpu.get_barrier_semaphore()
    peers = [{"z": up}, {"z": down}, {"xl": 1 - xl}]
    peers += [{"layer": lax.rem(me + k, layers)} for k in range(1, layers)]
    for peer in peers:
        pl.semaphore_signal(barrier, inc=1, device_id=peer, device_id_type=MESH)
    pl.semaphore_wait(barrier, len(peers))

    drains = []

    def stream(h):
        wide = h == 0
        kind = Wide if wide else Narrow
        here = pl.ds(h * tokens, tokens)

        inputs = kind(residual.at[h], res_send.at[h], res_recv.at[h], z, xl, turn)
        loads[h].wait()
        inputs.begin()
        yield

        if wide:
            loads[2].wait()
            loads[3].wait()

        def encode(blocks):
            total = preact[h]
            for block in blocks:
                rows = pl.ds(pl.multiple_of(block * width, width), width)
                total = total + jnp.dot(residual[h, block], encoder[rows, :], preferred_element_type=f32)
            preact[h] = total

        preact[h] = jnp.zeros((tokens, feats), f32) + enc_bias[...]
        encode([inputs.own])
        for phase in inputs.phases():
            encode(phase())
            yield
        codes[h] = jnp.maximum(preact[h], 0.0).astype(bf16)

        def code_copy(k):
            row = lax.rem(me + k, layers)
            wanted, slot = needs(row, me, layers)
            slot = jnp.where(wanted, slot, 0)
            copy = remote(codes.at[h], code_slots.at[h, slot], code_send.at[h, k], code_recv.at[h, slot], layer=row)
            return wanted, copy

        for k in range(1, layers):
            wanted, copy = code_copy(k)
            pl.when(wanted)(copy.start)

        @on_heavy
        def _():
            code_slots[h, me] = codes[h]

        @on_light
        def _():
            code_slots[h, slots - 1] = jnp.zeros((tokens, feats), bf16)

        yield
        for j in range(slots):
            copy = remote(codes.at[h], code_slots.at[h, j], code_send.at[h, 0], code_recv.at[h, j], layer=mirror)
            pl.when((j < all_slots) & (jnp.logical_not(heavy) | (me != j)))(copy.wait_recv)
        for j in range(slots):
            cols = pl.ds(j * feats, feats)
            block = code_slots[h, j]
            own = j < own_slots
            rows_in[h, 0, :, cols] = jnp.where(own, block, jnp.zeros_like(block))
            rows_in[h, 1, :, cols] = jnp.where(own, jnp.zeros_like(block), block)
        if wide:
            for load in loads[4:]:
                load.wait()

        def decode(a, block):
            cols = pl.ds(pl.multiple_of(block * width, width), width)
            part[h, a, block] = jnp.dot(rows_in[h, a], weights[:, cols], preferred_element_type=f32)

        def target(way, d):
            return around(z, jnp.where(way == 0, d, -d))

        def ring_copy(a, way, j, col):
            at = (h, a, way, j, col)
            return remote(
                ring_out.at[at], ring_in.at[at], ring_send.at[at], ring_recv.at[at], z=jnp.where(way == 0, up, down)
            )

        def cross_copy(a):
            return remote(cross_out.at[a], cross_in.at[a], cross_send.at[a], cross_recv.at[a], xl=1 - xl)

        def hand_copy(a, place):
            return remote(
                hand_out.at[a, place], hand_in.at[a, place], hand_send.at[a, place], hand_recv.at[a, place], xl=1 - xl
            )

        def ring_pieces(j):
            if wide:
                return [(way, col) for col in (0, 1) for way in (0, 1) if j > 0 or way == col]
            return [(turn, 0)] if j == 0 else [(turn, 0), (1 - turn, 0)]

        def block_of(way, d, col):
            return 2 * target(way, d) + (col if wide else xl)

        def hand_over(a):
            for place in [around(z, s) for s in (4, 3, -3, 2, -2, 1, -1, 0)]:
                block = 2 * place + 1 - xl
                decode(a, block)
                hand_out[a, place] = part[h, a, block].astype(bf16)
                hand_copy(a, place).start()

        def ring_decode(a, j):
            for way, col in ring_pieces(j):
                decode(a, block_of(way, 4 - j, col))

        def ring_step(a, j):
            before = ring_pieces(j - 1) if j else []
            for n, (way, col) in enumerate(ring_pieces(j)):
                place = target(way, 4 - j)
                value = part[h, a, block_of(way, 4 - j, col)]
                if not wide:
                    hand_copy(a, place).wait_recv()
                    value = value + hand_in[a, place].astype(f32)
                if (way, col) in before if wide else n < len(before):
                    ring_copy(a, way, j - 1, col).wait_recv()
                    value = value + ring_in[h, a, way, j - 1, col].astype(f32)
                ring_out[h, a, way, j, col] = value.astype(bf16)
                ring_copy(a, way, j, col).start()

        def ring_end(a):
            for col in (0, 1) if wide else (0,):
                for way in (0, 1):
                    ring_copy(a, way, 3, col).wait_recv()

            def total(block, col):
                both = ring_in[h, a, 0, 3, col].astype(f32) + ring_in[h, a, 1, 3, col].astype(f32)
                return part[h, a, block] + both

            if wide:
                cross_out[a] = total(2 * z + 1 - xl, 1 - xl).astype(bf16)
                cross_copy(a).start()
                part[h, a, mine] = total(mine, xl)
            else:
                hand_copy(a, z).wait_recv()
                part[h, a, mine] = total(mine, 0) + hand_in[a, z].astype(f32)

        def ring_sum(a):
            if wide:
                cross_copy(a).wait_recv()
                return part[h, a, mine] + cross_in[a].astype(f32)
            return part[h, a, mine]

        def mirror_copy():
            return remote(mirror_out.at[h], mirror_in.at[h], mirror_send.at[h], mirror_recv.at[h], layer=mirror)

        if not wide:
            on_heavy(lambda: hand_over(1))
            yield
            hand_over(0)
        for j in range(4):
            on_heavy(lambda: ring_decode(1, j))
            on_heavy(lambda: ring_step(1, j))
            yield
            ring_decode(0, j)
            ring_step(0, j)
            yield
        for a in (1, 0):
            def last(a=a):
                decode(a, mine)
                if wide:
                    decode(a, 2 * z + 1 - xl)
                ring_end(a)

            if a:
                on_heavy(last)
            else:
                last()
            yield

        @on_heavy
        def _():
            mirror_out[h] = ring_sum(1).astype(bf16)
            mirror_copy().start()

        yield
        bias = dec_bias[:, pl.ds(pl.multiple_of(mine * width, width), width)]
        part[h, 0, mine] = ring_sum(0) + bias - mlp[here, :].astype(f32)

        @on_light
        def _():
            mirror_copy().wait_recv()
            part[h, 0, mine] = part[h, 0, mine] + mirror_in[h].astype(f32)

        error = part[h, 0, mine].astype(bf16)
        err_ref[here, :] = error
        errors[h, 0, mine] = error

        first, second = [
            kind(errors.at[h, a], gather_send.at[h, a], gather_recv.at[h, a], z, xl, turn) for a in (0, 1)
        ]

        def back_copy():
            return remote(
                errors.at[h, 0, mine], errors.at[h, 1, mine], back_send.at[h], gather_recv.at[h, 1, mine], layer=mirror
            )

        on_light(lambda: back_copy().start())
        first.begin()
        yield
        early, late = first.phases(), second.phases()
        for phase in early[:3]:
            phase()
            yield

        @on_heavy
        def _():
            back_copy().wait_recv()
            second.begin()

        yield
        early[3]()
        yield
        on_heavy(lambda: late[0]() and None)
        yield
        early[4]()
        yield
        on_heavy(lambda: late[1]() and None)
        yield

        grad_ref[here, :] = jnp.zeros((tokens, feats), f32)

        def term_copy(j):
            source = jnp.where(j < own_slots, j, j + (half - 1) - me)
            return source, remote(
                terms_out.at[h, j], terms_in.at[h, me], term_send.at[h, j], term_recv.at[h, me], layer=source
            )

        def backward(a):
            def one(j, carry):
                rows = pl.ds(pl.multiple_of(j * feats, feats), feats)
                total = jnp.zeros((tokens, feats), f32)
                for block in range(2 * ZS):
                    total = total + lax.dot_general(
                        errors[h, a, block],
                        weights[rows, block * width : (block + 1) * width],
                        (((1,), (1,)), ((), ())),
                        preferred_element_type=f32,
                    )
                source, copy = term_copy(j)

                @pl.when(source == me)
                def _():
                    grad_ref[here, :] = total

                @pl.when(source != me)
                def _():
                    terms_out[h, j] = total.astype(bf16)
                    copy.start()

                return carry

            return one

        lax.fori_loop(0, own_slots, backward(0), 0)
        yield
        for phase in late[2:]:
            on_heavy(lambda phase=phase: phase() and None)
            yield

        @on_heavy
        def _():
            lax.fori_loop(own_slots, slots, backward(1), 0)

        yield

        def collect(row, carry):
            wanted, _ = needs(row, me, layers)

            @pl.when(wanted & (row != me))
            def _():
                remote(
                    terms_out.at[h, 0], terms_in.at[h, row], term_send.at[h, 0], term_recv.at[h, row], layer=mirror
                ).wait_recv()
                grad_ref[here, :] += terms_in[h, row].astype(f32)

            return carry

        lax.fori_loop(0, layers, collect, 0)

        def drain():
            inputs.drain()
            for k in range(1, layers):
                wanted, copy = code_copy(k)
                pl.when(wanted)(copy.wait_send)

            def drain_sums(a):
                for j in range(4):
                    for way, col in ring_pieces(j):
                        ring_copy(a, way, j, col).wait_send()
                if wide:
                    cross_copy(a).wait_send()
                else:
                    for place in range(ZS):
                        hand_copy(a, place).wait_send()

            drain_sums(0)
            first.drain()
            on_light(lambda: back_copy().wait_send())

            @on_heavy
            def _():
                drain_sums(1)
                mirror_copy().wait_send()
                second.drain()

            def drain_terms(j, carry):
                source, copy = term_copy(j)
                pl.when(source != me)(copy.wait_send)
                return carry

            lax.fori_loop(0, all_slots, drain_terms, 0)

        drains.append(drain)

    running = [stream(0), stream(1)]
    for _ in range(LEAD):
        next(running[0])
    while running:
        for s in list(running):
            try:
                next(s)
            except StopIteration:
                running.remove(s)
    for drain in drains:
        drain()


def shards(residual_in, mlp_out, encoder, encoder_bias, decoder, decoder_bias):
    layers = lax.axis_size("layer")
    tokens, width = residual_in.shape[1:]
    feats = encoder.shape[2]
    slots = decoder.shape[1]
    depth = decoder.shape[3]
    blocks = 2 * ZS
    part = tokens // 2
    bf16, f32 = jnp.bfloat16, jnp.float32
    dma, vmem = pltpu.SemaphoreType.DMA, pltpu.VMEM

    error, grad = pl.pallas_call(
        functools.partial(step_kernel, layers),
        out_shape=(
            jax.ShapeDtypeStruct((tokens, width), bf16),
            jax.ShapeDtypeStruct((tokens, feats), f32),
        ),
        in_specs=[pl.BlockSpec(memory_space=pltpu.HBM)] * 6,
        out_specs=(pl.BlockSpec(memory_space=vmem),) * 2,
        scratch_shapes=[
            vmem((2, blocks, part, width), bf16),
            vmem((tokens, width), bf16),
            vmem((depth, feats), bf16),
            vmem((1, feats), f32),
            vmem((slots * feats, depth), bf16),
            vmem((1, depth), f32),
            vmem((2, part, feats), f32),
            vmem((2, part, feats), bf16),
            vmem((2, slots, part, feats), bf16),
            vmem((2, 2, part, slots * feats), bf16),
            vmem((2, 2, blocks, part, width), f32),
            vmem((2, 2, 2, 4, 2, part, width), bf16),
            vmem((2, 2, 2, 4, 2, part, width), bf16),
            vmem((2, part, width), bf16),
            vmem((2, part, width), bf16),
            vmem((2, ZS, part, width), bf16),
            vmem((2, ZS, part, width), bf16),
            vmem((2, part, width), bf16),
            vmem((2, part, width), bf16),
            vmem((2, 2, blocks, part, width), bf16),
            vmem((2, slots, part, feats), bf16),
            vmem((2, layers, part, feats), bf16),
            dma((7,)),
            dma((2, 3, blocks)),
            dma((2, blocks)),
            dma((2, layers)),
            dma((2, slots)),
            dma((2, 2, 2, 4, 2)),
            dma((2, 2, 2, 4, 2)),
            dma((2,)),
            dma((2,)),
            dma((2, ZS)),
            dma((2, ZS)),
            dma((2,)),
            dma((2,)),
            dma((2,)),
            dma((2, 2, 3, blocks)),
            dma((2, 2, blocks)),
            dma((2, slots)),
            dma((2, layers)),
        ],
        compiler_params=pltpu.CompilerParams(
            collective_id=0, has_side_effects=True, vmem_limit_bytes=60 << 20
        ),
        name="transcoder_step",
    )(residual_in[0], mlp_out[0], encoder[0], encoder_bias, decoder[0].reshape(slots * feats, depth), decoder_bias)
    return error[None], grad[None]


def solution(mesh):
    split = Mesh(mesh.devices.reshape(mesh.shape["layer"], ZS, 2), ("layer", "z", "xl"))
    placed = (
        P("layer", None, FEAT),
        P("layer", None, FEAT),
        P("layer", None, FEAT),
        P("layer", FEAT),
        P("layer", None, FEAT, None),
        P("layer", None),
    )
    return jax.shard_map(
        shards,
        mesh=split,
        in_specs=placed,
        out_specs=(P("layer", None, FEAT), P("layer", None, FEAT)),
        check_vma=False,
    )
```

```python
import functools

import jax
import jax.numpy as jnp
from jax import lax
from jax.experimental import pallas as pl
from jax.experimental.pallas import tpu as pltpu
from jax.sharding import Mesh
from jax.sharding import PartitionSpec as P

MESH = pl.DeviceIdType.MESH
ZS = 8
FEAT = ("z", "xl")
ORDER = 25 * "AB" + "BAB"


def around(v, step):
    return lax.rem(v + step + ZS, ZS)


def remote(src, dst, send_sem, recv_sem, **where):
    return pltpu.make_async_remote_copy(
        src_ref=src, dst_ref=dst, send_sem=send_sem, recv_sem=recv_sem, device_id=where, device_id_type=MESH
    )


class Gather:
    def __init__(self, buf, send, recv, z, xl, turn):
        self.buf, self.send, self.recv, self.z, self.xl, self.turn = buf, send, recv, z, xl, turn
        self.own = 2 * z + xl
        self.other = 2 * z + 1 - xl
        self.up, self.down = around(z, 1), around(z, -1)

    def copy(self, way, block):
        where = ({"z": self.up}, {"z": self.down}, {"xl": 1 - self.xl})[way]
        at = self.buf.at[block]
        return remote(at, at, self.send, self.recv.at[block], **where)

    def push(self, way, block):
        self.copy(way, block).start()

    def arrive(self, block):
        self.copy(0, block).wait_recv()

    def begin(self):
        for way in (2, 0, 1):
            self.push(way, self.own)

    def drain(self):
        sent = self.buf.at[pl.ds(0, 2 * ZS - 1)]
        remote(sent, sent, self.send, self.recv.at[0], z=self.up).wait_send()


class Wide(Gather):
    def relay(self):
        self.arrive(self.other)
        for way in (0, 1):
            self.push(way, self.other)
        return [self.other]

    def blocks(self, d):
        out = []
        for col in (0, 1):
            for way in (0, 1):
                if d < 4 or way == col:
                    out.append((way, col, 2 * around(self.z, d if way else -d) + col))
        return out

    def step(self, d):
        for way, col, block in self.blocks(d):
            self.arrive(block)
            if d < 3 or (d == 3 and way == col):
                self.push(way, block)
        return [block for _, _, block in self.blocks(d)]

    def ready(self, n):
        return [block for _, _, block in self.blocks(n)] if n else [self.other]

    def phases(self):
        return [self.relay] + [functools.partial(self.step, d) for d in (1, 2, 3, 4)]


class Narrow(Gather):
    def blocks(self, d):
        if d == 4:
            return [(None, 2 * around(self.z, 4) + self.xl)]
        return [(way, 2 * around(self.z, d if way else -d) + self.xl) for way in (0, 1)]

    def crossed(self, d):
        places = [self.z] if d == 0 else [around(self.z, 4)] if d == 4 else [around(self.z, -d), around(self.z, d)]
        return [2 * place + 1 - self.xl for place in places]

    def step(self, d):
        out = []
        if d < 5:
            for way, block in self.blocks(d):
                self.arrive(block)
                if d < 3:
                    self.push(way, block)
                if d == 3:
                    pl.when(self.turn == way)(self.copy(way, block).start)
                self.push(2, block)
                out.append(block)
        for block in self.crossed(d - 1):
            self.arrive(block)
            out.append(block)
        return out

    def ready(self, n):
        return ([block for _, block in self.blocks(n + 1)] if n < 4 else []) + self.crossed(n)

    def phases(self):
        return [functools.partial(self.step, d) for d in (1, 2, 3, 4, 5)]


def needs(row, source, layers):
    half = layers // 2
    low = source < half
    wanted = (low & (row >= source)) | (jnp.logical_not(low) & (row <= layers - 1 - source))
    return wanted, jnp.where(low, source, source - (half - 1) + row)


def step_kernel(
    layers,
    res_ref,
    mlp_ref,
    enc_ref,
    enc_bias_ref,
    dec_ref,
    dec_bias_ref,
    err_ref,
    grad_ref,
    residual,
    mlp,
    encoder,
    enc_bias,
    weights,
    dec_bias,
    preact,
    codes,
    code_slots,
    rows_in,
    part,
    ring_out,
    ring_in,
    cross_out,
    cross_in,
    hand_out,
    hand_in,
    mirror_out,
    mirror_in,
    errors,
    sums,
    terms_out,
    terms_in,
    load_sem,
    res_send,
    res_recv,
    code_send,
    code_recv,
    ring_send,
    ring_recv,
    cross_send,
    cross_recv,
    hand_send,
    hand_recv,
    mirror_send,
    mirror_recv,
    back_send,
    gather_send,
    gather_recv,
    term_send,
    term_recv,
):
    half = layers // 2
    me, z, xl = lax.axis_index("layer"), lax.axis_index("z"), lax.axis_index("xl")
    _, slots, tokens, feats = code_slots.shape
    width = part.shape[4]
    bf16, f32 = jnp.bfloat16, jnp.float32
    heavy = me < half
    own_slots = jnp.where(heavy, me + 1, half)
    mirror = layers - 1 - me
    turn = lax.rem(me, 2)
    up, down = around(z, 1), around(z, -1)
    mine = 2 * z + xl
    on_heavy = pl.when(heavy)
    on_light = pl.when(jnp.logical_not(heavy))

    loads = [
        pltpu.make_async_copy(res_ref.at[pl.ds(h * tokens, tokens)], residual.at[h, mine], load_sem.at[h]) for h in (0, 1)
    ]
    loads += [
        pltpu.make_async_copy(enc_ref, encoder, load_sem.at[2]),
        pltpu.make_async_copy(enc_bias_ref, enc_bias, load_sem.at[3]),
        pltpu.make_async_copy(dec_ref, weights, load_sem.at[4]),
        pltpu.make_async_copy(mlp_ref, mlp, load_sem.at[5]),
        pltpu.make_async_copy(dec_bias_ref, dec_bias, load_sem.at[6]),
    ]
    for load in loads:
        load.start()

    barrier = pltpu.get_barrier_semaphore()
    peers = [{"z": up}, {"z": down}, {"xl": 1 - xl}]
    peers += [{"layer": lax.rem(me + k, layers)} for k in range(1, layers)]
    for peer in peers:
        pl.semaphore_signal(barrier, inc=1, device_id=peer, device_id_type=MESH)
    pl.semaphore_wait(barrier, len(peers))

    drains = []

    def stream(h):
        wide = h == 0
        kind = Wide if wide else Narrow
        here = pl.ds(h * tokens, tokens)

        inputs = kind(residual.at[h], res_send.at[h], res_recv.at[h], z, xl, turn)
        loads[h].wait()
        inputs.begin()
        yield

        if wide:
            loads[2].wait()
            loads[3].wait()

        def encode(blocks):
            total = preact[h]
            for block in blocks:
                rows = pl.ds(pl.multiple_of(block * width, width), width)
                total = total + jnp.dot(residual[h, block], encoder[rows, :], preferred_element_type=f32)
            preact[h] = total

        preact[h] = jnp.zeros((tokens, feats), f32) + enc_bias[...]
        encode([inputs.own])
        for n, phase in enumerate(inputs.phases()):
            encode(phase())
            if n < 4:
                yield
        codes[h] = jnp.maximum(preact[h], 0.0).astype(bf16)

        def code_copy(k):
            row = lax.rem(me + k, layers)
            wanted, slot = needs(row, me, layers)
            slot = jnp.where(wanted, slot, 0)
            copy = remote(codes.at[h], code_slots.at[h, slot], code_send.at[h, k], code_recv.at[h], layer=row)
            return wanted, copy

        for k in range(1, layers):
            wanted, copy = code_copy(k)
            pl.when(wanted)(copy.start)

        @on_heavy
        def _():
            code_slots[h, me] = codes[h]

        @on_light
        def _():
            code_slots[h, slots - 1] = jnp.zeros((tokens, feats), bf16)

        yield
        got = code_slots.at[h, pl.ds(0, half)]
        remote(got, got, code_send.at[h, 0], code_recv.at[h], layer=mirror).wait_recv()
        for j in range(slots):
            cols = pl.ds(j * feats, feats)
            block = code_slots[h, j]
            own = j < own_slots
            rows_in[h, 0:tokens, cols] = jnp.where(own, block, jnp.zeros_like(block))
            rows_in[h, tokens:, cols] = jnp.where(own, jnp.zeros_like(block), block)
        if wide:
            for load in loads[4:]:
                load.wait()

        def decode(blocks):
            def columns(block):
                return weights[:, pl.ds(pl.multiple_of(block * width, width), width)]

            @on_heavy
            def _():
                for block in blocks:
                    both = jnp.dot(rows_in[h], columns(block), preferred_element_type=f32)
                    part[h, 0, block] = both[:tokens]
                    part[h, 1, block] = both[tokens:]

            @on_light
            def _():
                for block in blocks:
                    part[h, 0, block] = jnp.dot(rows_in[h, 0:tokens, :], columns(block), preferred_element_type=f32)

        def target(way, d):
            return around(z, jnp.where(way == 0, d, -d))

        def ring_copy(a, way, j, col):
            at = (h, a, way, j, col)
            return remote(
                ring_out.at[at], ring_in.at[at], ring_send.at[h, a], ring_recv.at[at], z=jnp.where(way == 0, up, down)
            )

        def cross_copy(a):
            return remote(cross_out.at[a], cross_in.at[a], cross_send.at[a], cross_recv.at[a], xl=1 - xl)

        def hand_copy(a, place):
            return remote(
                hand_out.at[a, place], hand_in.at[a, place], hand_send.at[a], hand_recv.at[a, place], xl=1 - xl
            )

        def ring_pieces(j):
            if wide:
                return [(way, col) for col in (0, 1) for way in (0, 1) if j > 0 or way == col]
            return [(turn, 0)] if j == 0 else [(turn, 0), (1 - turn, 0)]

        def block_of(way, d, col):
            return 2 * target(way, d) + (col if wide else xl)

        def hand_over(steps):
            places = [around(z, s) for s in steps]
            decode([2 * place + 1 - xl for place in places])

            def send(a):
                for place in places:
                    hand_out[a, place] = part[h, a, 2 * place + 1 - xl].astype(bf16)
                    hand_copy(a, place).start()

            on_heavy(lambda: send(1))
            send(0)

        def ring_decode(j):
            decode([block_of(way, 4 - j, col) for way, col in ring_pieces(j)])

        def ring_step(a, j):
            before = ring_pieces(j - 1) if j else []
            for n, (way, col) in enumerate(ring_pieces(j)):
                place = target(way, 4 - j)
                value = part[h, a, block_of(way, 4 - j, col)]
                if not wide:
                    hand_copy(a, place).wait_recv()
                    value = value + hand_in[a, place].astype(f32)
                if (way, col) in before if wide else n < len(before):
                    ring_copy(a, way, j - 1, col).wait_recv()
                    value = value + ring_in[h, a, way, j - 1, col].astype(f32)
                ring_out[h, a, way, j, col] = value.astype(bf16)
                ring_copy(a, way, j, col).start()

        def ring_end(a):
            for col in (0, 1) if wide else (0,):
                for way in (0, 1):
                    ring_copy(a, way, 3, col).wait_recv()

            def total(block, col):
                both = ring_in[h, a, 0, 3, col].astype(f32) + ring_in[h, a, 1, 3, col].astype(f32)
                return part[h, a, block] + both

            if wide:
                cross_out[a] = total(2 * z + 1 - xl, 1 - xl).astype(bf16)
                cross_copy(a).start()
                part[h, a, mine] = total(mine, xl)
            else:
                hand_copy(a, z).wait_recv()
                part[h, a, mine] = total(mine, 0) + hand_in[a, z].astype(f32)

        def ring_sum(a):
            if wide:
                cross_copy(a).wait_recv()
                return part[h, a, mine] + cross_in[a].astype(f32)
            return part[h, a, mine]

        def mirror_copy():
            return remote(mirror_out.at[h], mirror_in.at[h], mirror_send.at[h], mirror_recv.at[h], layer=mirror)

        if not wide:
            hand_over((4, 3, -3))
            yield
            hand_over((2, -2, 1, -1, 0))
        for j in range(4):
            ring_decode(j)
            on_heavy(lambda: ring_step(1, j))
            ring_step(0, j)
            yield
        decode([mine, 2 * z + 1 - xl] if wide else [mine])
        on_heavy(lambda: ring_end(1))
        ring_end(0)
        yield

        @on_heavy
        def _():
            mirror_out[h] = ring_sum(1).astype(bf16)
            mirror_copy().start()

        yield
        bias = dec_bias[:, pl.ds(pl.multiple_of(mine * width, width), width)]
        part[h, 0, mine] = ring_sum(0) + bias - mlp[here, :].astype(f32)

        @on_light
        def _():
            mirror_copy().wait_recv()
            part[h, 0, mine] = part[h, 0, mine] + mirror_in[h].astype(f32)

        error = part[h, 0, mine].astype(bf16)
        err_ref[here, :] = error
        errors[h, 0, mine] = error

        first, second = [
            kind(errors.at[h, a], gather_send.at[h, a], gather_recv.at[h, a], z, xl, turn) for a in (0, 1)
        ]

        def back_copy():
            return remote(
                errors.at[h, 0, mine], errors.at[h, 1, mine], back_send.at[h], gather_recv.at[h, 1, mine], layer=mirror
            )

        on_light(lambda: back_copy().start())
        first.begin()
        yield
        def term_copy(j):
            source = jnp.where(j < own_slots, j, j + (half - 1) - me)
            return source, remote(
                terms_out.at[h, j], terms_in.at[h, me], term_send.at[h], term_recv.at[h, me], layer=source
            )

        def backward(a, blocks, start, end):
            def one(j, carry):
                rows = pl.ds(pl.multiple_of(j * feats, feats), feats)
                total = jnp.zeros((tokens, feats), f32) if start else sums[h, j]
                for block in blocks:
                    cols = pl.ds(pl.multiple_of(block * width, width), width)
                    total = total + lax.dot_general(
                        errors[h, a, block],
                        weights[rows, cols],
                        (((1,), (1,)), ((), ())),
                        preferred_element_type=f32,
                    )
                if not end:
                    sums[h, j] = total
                    return carry
                source, copy = term_copy(j)

                @pl.when(source == me)
                def _():
                    grad_ref[here, :] = total

                @pl.when(source != me)
                def _():
                    terms_out[h, j] = total.astype(bf16)
                    copy.start()

                return carry

            lax.fori_loop(own_slots if a else 0, slots if a else own_slots, one, 0)

        grad_ref[here, :] = jnp.zeros((tokens, feats), f32)
        early, late = first.phases(), second.phases()
        for phase in early[:3]:
            phase()
            yield

        @on_heavy
        def _():
            back_copy().wait_recv()
            second.begin()

        yield
        early[3]()
        yield

        @on_heavy
        def _():
            late[0]()

        yield
        early[4]()
        yield

        @on_heavy
        def _():
            late[1]()
            backward(1, [second.own] + second.ready(0) + second.ready(1), True, False)

        yield
        backward(0, list(range(2 * ZS)), True, True)
        yield

        @on_heavy
        def _():
            late[2]()

        yield

        @on_heavy
        def _():
            late[3]()
            backward(1, second.ready(2) + second.ready(3), False, False)

        yield

        @on_heavy
        def _():
            backward(1, late[4](), False, True)

        yield

        def collect(row, carry):
            wanted, _ = needs(row, me, layers)

            @pl.when(wanted & (row != me))
            def _():
                remote(
                    terms_out.at[h, 0], terms_in.at[h, row], term_send.at[h], term_recv.at[h, row], layer=mirror
                ).wait_recv()
                grad_ref[here, :] += terms_in[h, row].astype(f32)

            return carry

        lax.fori_loop(0, layers, collect, 0)

        def drain():
            inputs.drain()
            for k in range(1, layers):
                wanted, copy = code_copy(k)
                pl.when(wanted)(copy.wait_send)

            def drain_sums(a):
                sent = residual.at[h, pl.ds(0, 14 if wide else 7)]
                remote(sent, sent, ring_send.at[h, a], ring_recv.at[h, a, 0, 0, 0], z=up).wait_send()
                if wide:
                    cross_copy(a).wait_send()
                else:
                    sent = hand_out.at[a]
                    remote(sent, sent, hand_send.at[a], hand_recv.at[a, 0], xl=1 - xl).wait_send()

            drain_sums(0)
            first.drain()
            on_light(lambda: back_copy().wait_send())

            @on_heavy
            def _():
                drain_sums(1)
                mirror_copy().wait_send()
                second.drain()

            sent = terms_out.at[h, pl.ds(0, half)]
            remote(sent, sent, term_send.at[h], term_recv.at[h, 0], layer=mirror).wait_send()

        drains.append(drain)

    running = {"A": stream(0), "B": stream(1)}
    for name in ORDER + 40 * "AB":
        if name in running and next(running[name], "end") == "end":
            del running[name]
    for drain in drains:
        drain()


def shards(residual_in, mlp_out, encoder, encoder_bias, decoder, decoder_bias):
    layers = lax.axis_size("layer")
    tokens, width = residual_in.shape[1:]
    feats = encoder.shape[2]
    slots = decoder.shape[1]
    depth = decoder.shape[3]
    blocks = 2 * ZS
    part = tokens // 2
    bf16, f32 = jnp.bfloat16, jnp.float32
    dma, vmem = pltpu.SemaphoreType.DMA, pltpu.VMEM

    error, grad = pl.pallas_call(
        functools.partial(step_kernel, layers),
        out_shape=(
            jax.ShapeDtypeStruct((tokens, width), bf16),
            jax.ShapeDtypeStruct((tokens, feats), f32),
        ),
        in_specs=[pl.BlockSpec(memory_space=pltpu.HBM)] * 6,
        out_specs=(pl.BlockSpec(memory_space=vmem),) * 2,
        scratch_shapes=[
            vmem((2, blocks, part, width), bf16),
            vmem((tokens, width), bf16),
            vmem((depth, feats), bf16),
            vmem((1, feats), f32),
            vmem((slots * feats, depth), bf16),
            vmem((1, depth), f32),
            vmem((2, part, feats), f32),
            vmem((2, part, feats), bf16),
            vmem((2, slots, part, feats), bf16),
            vmem((2, tokens, slots * feats), bf16),
            vmem((2, 2, blocks, part, width), f32),
            vmem((2, 2, 2, 4, 2, part, width), bf16),
            vmem((2, 2, 2, 4, 2, part, width), bf16),
            vmem((2, part, width), bf16),
            vmem((2, part, width), bf16),
            vmem((2, ZS, part, width), bf16),
            vmem((2, ZS, part, width), bf16),
            vmem((2, part, width), bf16),
            vmem((2, part, width), bf16),
            vmem((2, 2, blocks, part, width), bf16),
            vmem((2, slots, part, feats), f32),
            vmem((2, slots, part, feats), bf16),
            vmem((2, layers, part, feats), bf16),
            dma((7,)),
            dma((2,)),
            dma((2, blocks)),
            dma((2, layers)),
            dma((2,)),
            dma((2, 2)),
            dma((2, 2, 2, 4, 2)),
            dma((2,)),
            dma((2,)),
            dma((2,)),
            dma((2, ZS)),
            dma((2,)),
            dma((2,)),
            dma((2,)),
            dma((2, 2)),
            dma((2, 2, blocks)),
            dma((2,)),
            dma((2, layers)),
        ],
        compiler_params=pltpu.CompilerParams(
            collective_id=0, has_side_effects=True, vmem_limit_bytes=60 << 20
        ),
        name="transcoder_step",
    )(residual_in[0], mlp_out[0], encoder[0], encoder_bias, decoder[0].reshape(slots * feats, depth), decoder_bias)
    return error[None], grad[None]


def solution(mesh):
    split = Mesh(mesh.devices.reshape(mesh.shape["layer"], ZS, 2), ("layer", "z", "xl"))
    placed = (
        P("layer", None, FEAT),
        P("layer", None, FEAT),
        P("layer", None, FEAT),
        P("layer", FEAT),
        P("layer", None, FEAT, None),
        P("layer", None),
    )
    return jax.shard_map(
        shards,
        mesh=split,
        in_specs=placed,
        out_specs=(P("layer", None, FEAT), P("layer", None, FEAT)),
        check_vma=False,
    )
```

```python
import functools

import jax
import jax.numpy as jnp
from jax import lax
from jax.experimental import pallas as pl
from jax.experimental.pallas import tpu as pltpu
from jax.sharding import Mesh
from jax.sharding import PartitionSpec as P

MESH = pl.DeviceIdType.MESH
ZS = 8
FEAT = ("z", "xl")
ORDER = 11 * "AB" + "AABB" + 12 * "AB" + "BAB"


def around(v, step):
    return lax.rem(v + step + ZS, ZS)


def remote(src, dst, send_sem, recv_sem, **where):
    return pltpu.make_async_remote_copy(
        src_ref=src, dst_ref=dst, send_sem=send_sem, recv_sem=recv_sem, device_id=where, device_id_type=MESH
    )


class Gather:
    def __init__(self, buf, send, recv, z, xl, turn):
        self.buf, self.send, self.recv, self.z, self.xl, self.turn = buf, send, recv, z, xl, turn
        self.own = 2 * z + xl
        self.other = 2 * z + 1 - xl
        self.up, self.down = around(z, 1), around(z, -1)

    def copy(self, way, block):
        where = ({"z": self.up}, {"z": self.down}, {"xl": 1 - self.xl})[way]
        at = self.buf.at[block]
        return remote(at, at, self.send, self.recv.at[block], **where)

    def push(self, way, block):
        self.copy(way, block).start()

    def arrive(self, block):
        self.copy(0, block).wait_recv()

    def begin(self):
        for way in (2, 0, 1):
            self.push(way, self.own)

    def drain(self):
        sent = self.buf.at[pl.ds(0, 2 * ZS - 1)]
        remote(sent, sent, self.send, self.recv.at[0], z=self.up).wait_send()


class Wide(Gather):
    def relay(self):
        self.arrive(self.other)
        for way in (0, 1):
            self.push(way, self.other)
        return [self.other]

    def blocks(self, d):
        out = []
        for col in (0, 1):
            for way in (0, 1):
                if d < 4 or way == col:
                    out.append((way, col, 2 * around(self.z, d if way else -d) + col))
        return out

    def step(self, d):
        for way, col, block in self.blocks(d):
            self.arrive(block)
            if d < 3 or (d == 3 and way == col):
                self.push(way, block)
        return [block for _, _, block in self.blocks(d)]

    def ready(self, n):
        return [block for _, _, block in self.blocks(n)] if n else [self.other]

    def phases(self):
        return [self.relay] + [functools.partial(self.step, d) for d in (1, 2, 3, 4)]


class Narrow(Gather):
    def begin(self):
        for way in (0, 1):
            self.push(way, self.own)

    def blocks(self, d):
        if d == 4:
            return [(None, 2 * around(self.z, 4) + self.xl)]
        return [(way, 2 * around(self.z, d if way else -d) + self.xl) for way in (0, 1)]

    def crossed(self, d):
        places = [self.z] if d == 0 else [around(self.z, 4)] if d == 4 else [around(self.z, -d), around(self.z, d)]
        return [2 * place + 1 - self.xl for place in places]

    def step(self, d):
        out = []
        if d == 1:
            self.push(2, self.own)
        if d < 5:
            for way, block in self.blocks(d):
                self.arrive(block)
                if d < 3:
                    self.push(way, block)
                if d == 3:
                    pl.when(self.turn == way)(self.copy(way, block).start)
                self.push(2, block)
                out.append(block)
        for block in self.crossed(d - 1):
            self.arrive(block)
            out.append(block)
        return out

    def ready(self, n):
        return ([block for _, block in self.blocks(n + 1)] if n < 4 else []) + self.crossed(n)

    def phases(self):
        return [functools.partial(self.step, d) for d in (1, 2, 3, 4, 5)]


def needs(row, source, layers):
    half = layers // 2
    low = source < half
    wanted = (low & (row >= source)) | (jnp.logical_not(low) & (row <= layers - 1 - source))
    return wanted, jnp.where(low, source, source - (half - 1) + row)


def step_kernel(
    layers,
    res_ref,
    mlp_ref,
    enc_ref,
    enc_bias_ref,
    dec_ref,
    dec_bias_ref,
    err_ref,
    grad_ref,
    residual,
    mlp,
    encoder,
    enc_bias,
    weights,
    dec_bias,
    preact,
    codes,
    code_slots,
    rows_in,
    part,
    ring_out,
    ring_in,
    cross_out,
    cross_in,
    hand_out,
    hand_in,
    mirror_out,
    mirror_in,
    errors,
    sums,
    terms_out,
    terms_in,
    load_sem,
    res_send,
    res_recv,
    code_send,
    relay_send,
    code_recv,
    ring_send,
    ring_recv,
    cross_send,
    cross_recv,
    hand_send,
    hand_recv,
    mirror_send,
    mirror_recv,
    back_send,
    gather_send,
    gather_recv,
    term_send,
    term_recv,
):
    half = layers // 2
    me, z, xl = lax.axis_index("layer"), lax.axis_index("z"), lax.axis_index("xl")
    _, slots, tokens, feats = code_slots.shape
    width = part.shape[4]
    bf16, f32 = jnp.bfloat16, jnp.float32
    heavy = me < half
    own_slots = jnp.where(heavy, me + 1, half)
    mirror = layers - 1 - me
    turn = lax.rem(me, 2)
    up, down = around(z, 1), around(z, -1)
    mine = 2 * z + xl
    on_heavy = pl.when(heavy)
    on_light = pl.when(jnp.logical_not(heavy))

    loads = [
        pltpu.make_async_copy(res_ref.at[pl.ds(h * tokens, tokens)], residual.at[h, mine], load_sem.at[h]) for h in (0, 1)
    ]
    loads += [
        pltpu.make_async_copy(enc_ref, encoder, load_sem.at[2]),
        pltpu.make_async_copy(enc_bias_ref, enc_bias, load_sem.at[3]),
        pltpu.make_async_copy(dec_ref, weights, load_sem.at[4]),
        pltpu.make_async_copy(mlp_ref, mlp, load_sem.at[5]),
        pltpu.make_async_copy(dec_bias_ref, dec_bias, load_sem.at[6]),
    ]
    for load in loads:
        load.start()

    barrier = pltpu.get_barrier_semaphore()
    peers = [{"z": up}, {"z": down}, {"xl": 1 - xl}]
    peers += [{"layer": lax.rem(me + k, layers)} for k in range(1, layers)]
    for peer in peers:
        pl.semaphore_signal(barrier, inc=1, device_id=peer, device_id_type=MESH)
    pl.semaphore_wait(barrier, len(peers))

    drains = []

    def stream(h):
        wide = h == 0
        kind = Wide if wide else Narrow
        here = pl.ds(h * tokens, tokens)

        inputs = kind(residual.at[h], res_send.at[h], res_recv.at[h], z, xl, turn)
        loads[h].wait()
        inputs.begin()
        yield

        if wide:
            loads[2].wait()
            loads[3].wait()

        def encode(blocks):
            total = preact[h]
            for block in blocks:
                rows = pl.ds(pl.multiple_of(block * width, width), width)
                total = total + jnp.dot(residual[h, block], encoder[rows, :], preferred_element_type=f32)
            preact[h] = total

        preact[h] = jnp.zeros((tokens, feats), f32) + enc_bias[...]
        encode([inputs.own])
        for n, phase in enumerate(inputs.phases()):
            encode(phase())
            if n < 4:
                yield
        codes[h] = jnp.maximum(preact[h], 0.0).astype(bf16)

        def code_copy(k):
            chip = lax.rem(me // 2 + k, half)
            row = 2 * chip + jnp.where(heavy, 1, 0)
            wanted, slot = needs(row, me, layers)
            wanted = wanted & (row != me)
            slot = jnp.where(wanted, slot, 0)
            copy = remote(codes.at[h], code_slots.at[h, slot], code_send.at[h, k], code_recv.at[h, slot], layer=row)
            return wanted, copy

        def code_relay(n):
            source = n + half * (1 - turn)
            here, slot = needs(me, source, layers)
            here = here & (source != me)
            slot = jnp.where(here, slot, 0)
            partner = me + 1 - 2 * turn
            there, far = needs(partner, source, layers)
            there = here & there & (source != partner)
            far = jnp.where(there, far, 0)
            copy = remote(
                code_slots.at[h, slot], code_slots.at[h, far], relay_send.at[h, n], code_recv.at[h, far], layer=partner
            )
            return here, slot, there, copy

        def code_wait(slot):
            at = code_slots.at[h, slot]
            return remote(at, at, code_send.at[h, 0], code_recv.at[h, slot], layer=mirror).wait_recv

        for k in range(half):
            wanted, copy = code_copy(k)
            pl.when(wanted)(copy.start)

        @on_heavy
        def _():
            code_slots[h, me] = codes[h]

        @on_light
        def _():
            code_slots[h, slots - 1] = jnp.zeros((tokens, feats), bf16)

        yield
        for n in range(half):
            arrived, slot, there, copy = code_relay(n)
            pl.when(arrived)(code_wait(slot))
            pl.when(there)(copy.start)
        for n in range(half):
            source = n + half * turn
            arrived, slot = needs(me, source, layers)
            arrived = arrived & (source != me)
            pl.when(arrived)(code_wait(jnp.where(arrived, slot, 0)))
        for j in range(slots):
            cols = pl.ds(j * feats, feats)
            block = code_slots[h, j]
            own = j < own_slots
            rows_in[h, 0:tokens, cols] = jnp.where(own, block, jnp.zeros_like(block))
            rows_in[h, tokens:, cols] = jnp.where(own, jnp.zeros_like(block), block)
        if wide:
            for load in loads[4:]:
                load.wait()

        def decode(blocks):
            def columns(block):
                return weights[:, pl.ds(pl.multiple_of(block * width, width), width)]

            @on_heavy
            def _():
                for block in blocks:
                    both = jnp.dot(rows_in[h], columns(block), preferred_element_type=f32)
                    part[h, 0, block] = both[:tokens]
                    part[h, 1, block] = both[tokens:]

            @on_light
            def _():
                for block in blocks:
                    part[h, 0, block] = jnp.dot(rows_in[h, 0:tokens, :], columns(block), preferred_element_type=f32)

        def target(way, d):
            return around(z, jnp.where(way == 0, d, -d))

        def ring_copy(a, way, j, col):
            at = (h, a, way, j, col)
            return remote(
                ring_out.at[at], ring_in.at[at], ring_send.at[h, a], ring_recv.at[at], z=jnp.where(way == 0, up, down)
            )

        def cross_copy(a):
            return remote(cross_out.at[a], cross_in.at[a], cross_send.at[a], cross_recv.at[a], xl=1 - xl)

        def hand_copy(a, place):
            return remote(
                hand_out.at[a, place], hand_in.at[a, place], hand_send.at[a], hand_recv.at[a, place], xl=1 - xl
            )

        def ring_pieces(j):
            if wide:
                return [(way, col) for col in (0, 1) for way in (0, 1) if j > 0 or way == col]
            return [(turn, 0)] if j == 0 else [(turn, 0), (1 - turn, 0)]

        def block_of(way, d, col):
            return 2 * target(way, d) + (col if wide else xl)

        def hand_over(steps):
            places = [around(z, s) for s in steps]
            decode([2 * place + 1 - xl for place in places])

            def send(a):
                for place in places:
                    hand_out[a, place] = part[h, a, 2 * place + 1 - xl].astype(bf16)
                    hand_copy(a, place).start()

            on_heavy(lambda: send(1))
            send(0)

        def ring_decode(j):
            decode([block_of(way, 4 - j, col) for way, col in ring_pieces(j)])

        def ring_step(a, j):
            before = ring_pieces(j - 1) if j else []
            for n, (way, col) in enumerate(ring_pieces(j)):
                place = target(way, 4 - j)
                value = part[h, a, block_of(way, 4 - j, col)]
                if not wide:
                    hand_copy(a, place).wait_recv()
                    value = value + hand_in[a, place].astype(f32)
                if (way, col) in before if wide else n < len(before):
                    ring_copy(a, way, j - 1, col).wait_recv()
                    value = value + ring_in[h, a, way, j - 1, col].astype(f32)
                ring_out[h, a, way, j, col] = value.astype(bf16)
                ring_copy(a, way, j, col).start()

        def ring_end(a):
            for col in (0, 1) if wide else (0,):
                for way in (0, 1):
                    ring_copy(a, way, 3, col).wait_recv()

            def total(block, col):
                both = ring_in[h, a, 0, 3, col].astype(f32) + ring_in[h, a, 1, 3, col].astype(f32)
                return part[h, a, block] + both

            if wide:
                cross_out[a] = total(2 * z + 1 - xl, 1 - xl).astype(bf16)
                cross_copy(a).start()
                part[h, a, mine] = total(mine, xl)
            else:
                hand_copy(a, z).wait_recv()
                part[h, a, mine] = total(mine, 0) + hand_in[a, z].astype(f32)

        def ring_sum(a):
            if wide:
                cross_copy(a).wait_recv()
                return part[h, a, mine] + cross_in[a].astype(f32)
            return part[h, a, mine]

        def mirror_copy():
            return remote(mirror_out.at[h], mirror_in.at[h], mirror_send.at[h], mirror_recv.at[h], layer=mirror)

        if not wide:
            hand_over((4, 3, -3))
            yield
            hand_over((2, -2, 1, -1, 0))
        for j in range(4):
            ring_decode(j)
            on_heavy(lambda: ring_step(1, j))
            ring_step(0, j)
            yield
        decode([mine, 2 * z + 1 - xl] if wide else [mine])
        on_heavy(lambda: ring_end(1))
        ring_end(0)
        yield

        @on_heavy
        def _():
            mirror_out[h] = ring_sum(1).astype(bf16)
            mirror_copy().start()

        yield
        bias = dec_bias[:, pl.ds(pl.multiple_of(mine * width, width), width)]
        part[h, 0, mine] = ring_sum(0) + bias - mlp[here, :].astype(f32)

        @on_light
        def _():
            mirror_copy().wait_recv()
            part[h, 0, mine] = part[h, 0, mine] + mirror_in[h].astype(f32)

        error = part[h, 0, mine].astype(bf16)
        err_ref[here, :] = error
        errors[h, 0, mine] = error

        first, second = [
            kind(errors.at[h, a], gather_send.at[h, a], gather_recv.at[h, a], z, xl, turn) for a in (0, 1)
        ]

        def back_copy():
            return remote(
                errors.at[h, 0, mine], errors.at[h, 1, mine], back_send.at[h], gather_recv.at[h, 1, mine], layer=mirror
            )

        on_light(lambda: back_copy().start())
        first.begin()
        yield
        def term_copy(j):
            source = jnp.where(j < own_slots, j, j + (half - 1) - me)
            return source, remote(
                terms_out.at[h, j], terms_in.at[h, me], term_send.at[h], term_recv.at[h, me], layer=source
            )

        def backward(a, blocks, start, end):
            def one(j, carry):
                rows = pl.ds(pl.multiple_of(j * feats, feats), feats)
                total = jnp.zeros((tokens, feats), f32) if start else sums[h, j]
                for block in blocks:
                    cols = pl.ds(pl.multiple_of(block * width, width), width)
                    total = total + lax.dot_general(
                        errors[h, a, block],
                        weights[rows, cols],
                        (((1,), (1,)), ((), ())),
                        preferred_element_type=f32,
                    )
                if not end:
                    sums[h, j] = total
                    return carry
                source, copy = term_copy(j)

                @pl.when(source == me)
                def _():
                    grad_ref[here, :] = total

                @pl.when(source != me)
                def _():
                    terms_out[h, j] = total.astype(bf16)
                    copy.start()

                return carry

            lax.fori_loop(own_slots if a else 0, slots if a else own_slots, one, 0)

        grad_ref[here, :] = jnp.zeros((tokens, feats), f32)
        early, late = first.phases(), second.phases()
        for phase in early[:2]:
            phase()
            yield

        @on_heavy
        def _():
            back_copy().wait_recv()
            second.begin()

        yield
        early[2]()
        yield

        @on_heavy
        def _():
            late[0]()

        yield
        early[3]()
        yield

        @on_heavy
        def _():
            late[1]()
            backward(1, [second.own] + second.ready(0) + second.ready(1), True, False)

        yield
        early[4]()
        yield

        @on_heavy
        def _():
            late[2]()

        yield
        backward(0, list(range(2 * ZS)), True, True)
        yield

        @on_heavy
        def _():
            late[3]()
            backward(1, second.ready(2) + second.ready(3), False, False)

        yield

        @on_heavy
        def _():
            backward(1, late[4](), False, True)

        yield

        def collect(row, carry):
            wanted, _ = needs(row, me, layers)

            @pl.when(wanted & (row != me))
            def _():
                remote(
                    terms_out.at[h, 0], terms_in.at[h, row], term_send.at[h], term_recv.at[h, row], layer=mirror
                ).wait_recv()
                grad_ref[here, :] += terms_in[h, row].astype(f32)

            return carry

        lax.fori_loop(0, layers, collect, 0)

        def drain():
            inputs.drain()
            for k in range(half):
                wanted, copy = code_copy(k)
                pl.when(wanted)(copy.wait_send)
                _, _, there, copy = code_relay(k)
                pl.when(there)(copy.wait_send)

            def drain_sums(a):
                sent = residual.at[h, pl.ds(0, 14 if wide else 7)]
                remote(sent, sent, ring_send.at[h, a], ring_recv.at[h, a, 0, 0, 0], z=up).wait_send()
                if wide:
                    cross_copy(a).wait_send()
                else:
                    sent = hand_out.at[a]
                    remote(sent, sent, hand_send.at[a], hand_recv.at[a, 0], xl=1 - xl).wait_send()

            drain_sums(0)
            first.drain()
            on_light(lambda: back_copy().wait_send())

            @on_heavy
            def _():
                drain_sums(1)
                mirror_copy().wait_send()
                second.drain()

            sent = terms_out.at[h, pl.ds(0, half)]
            remote(sent, sent, term_send.at[h], term_recv.at[h, 0], layer=mirror).wait_send()

        drains.append(drain)

    running = {"A": stream(0), "B": stream(1)}
    for name in ORDER + 40 * "AB":
        if name in running and next(running[name], "end") == "end":
            del running[name]
    for drain in drains:
        drain()


def shards(residual_in, mlp_out, encoder, encoder_bias, decoder, decoder_bias):
    layers = lax.axis_size("layer")
    tokens, width = residual_in.shape[1:]
    feats = encoder.shape[2]
    slots = decoder.shape[1]
    depth = decoder.shape[3]
    blocks = 2 * ZS
    part = tokens // 2
    bf16, f32 = jnp.bfloat16, jnp.float32
    dma, vmem = pltpu.SemaphoreType.DMA, pltpu.VMEM

    error, grad = pl.pallas_call(
        functools.partial(step_kernel, layers),
        out_shape=(
            vmem((tokens, width), bf16),
            vmem((tokens, feats), f32),
        ),
        in_specs=[pl.BlockSpec(memory_space=pltpu.HBM)] * 6,
        out_specs=(pl.BlockSpec(memory_space=vmem),) * 2,
        scratch_shapes=[
            vmem((2, blocks, part, width), bf16),
            vmem((tokens, width), bf16),
            vmem((depth, feats), bf16),
            vmem((1, feats), f32),
            vmem((slots * feats, depth), bf16),
            vmem((1, depth), f32),
            vmem((2, part, feats), f32),
            vmem((2, part, feats), bf16),
            vmem((2, slots, part, feats), bf16),
            vmem((2, tokens, slots * feats), bf16),
            vmem((2, 2, blocks, part, width), f32),
            vmem((2, 2, 2, 4, 2, part, width), bf16),
            vmem((2, 2, 2, 4, 2, part, width), bf16),
            vmem((2, part, width), bf16),
            vmem((2, part, width), bf16),
            vmem((2, ZS, part, width), bf16),
            vmem((2, ZS, part, width), bf16),
            vmem((2, part, width), bf16),
            vmem((2, part, width), bf16),
            vmem((2, 2, blocks, part, width), bf16),
            vmem((2, slots, part, feats), f32),
            vmem((2, slots, part, feats), bf16),
            vmem((2, layers, part, feats), bf16),
            dma((7,)),
            dma((2,)),
            dma((2, blocks)),
            dma((2, layers // 2)),
            dma((2, layers // 2)),
            dma((2, slots)),
            dma((2, 2)),
            dma((2, 2, 2, 4, 2)),
            dma((2,)),
            dma((2,)),
            dma((2,)),
            dma((2, ZS)),
            dma((2,)),
            dma((2,)),
            dma((2,)),
            dma((2, 2)),
            dma((2, 2, blocks)),
            dma((2,)),
            dma((2, layers)),
        ],
        compiler_params=pltpu.CompilerParams(
            collective_id=0, has_side_effects=True, vmem_limit_bytes=60 << 20
        ),
        name="transcoder_step",
    )(residual_in[0], mlp_out[0], encoder[0], encoder_bias, decoder[0].reshape(slots * feats, depth), decoder_bias)
    return error[None], grad[None]


def solution(mesh):
    split = Mesh(mesh.devices.reshape(mesh.shape["layer"], ZS, 2), ("layer", "z", "xl"))
    placed = (
        P("layer", None, FEAT),
        P("layer", None, FEAT),
        P("layer", None, FEAT),
        P("layer", FEAT),
        P("layer", None, FEAT, None),
        P("layer", None),
    )
    return jax.shard_map(
        shards,
        mesh=split,
        in_specs=placed,
        out_specs=(P("layer", None, FEAT), P("layer", None, FEAT)),
        check_vma=False,
    )
```

```python
import functools

import jax
import jax.numpy as jnp
from jax import lax
from jax.experimental import pallas as pl
from jax.experimental.pallas import tpu as pltpu
from jax.sharding import Mesh
from jax.sharding import PartitionSpec as P

MESH = pl.DeviceIdType.MESH
ZS = 8
FEAT = ("z", "xl")
ORDER = 11 * "AB" + "AABB" + 12 * "AB" + "BAB"


def around(v, step):
    return lax.rem(v + step + ZS, ZS)


def remote(src, dst, send_sem, recv_sem, **where):
    return pltpu.make_async_remote_copy(
        src_ref=src, dst_ref=dst, send_sem=send_sem, recv_sem=recv_sem, device_id=where, device_id_type=MESH
    )


class Gather:
    def __init__(self, buf, send, recv, z, xl, turn):
        self.buf, self.send, self.recv, self.z, self.xl, self.turn = buf, send, recv, z, xl, turn
        self.own = 2 * z + xl
        self.other = 2 * z + 1 - xl
        self.up, self.down = around(z, 1), around(z, -1)

    def copy(self, way, block):
        where = ({"z": self.up}, {"z": self.down}, {"xl": 1 - self.xl})[way]
        at = self.buf.at[block]
        return remote(at, at, self.send, self.recv.at[block], **where)

    def push(self, way, block):
        self.copy(way, block).start()

    def arrive(self, block):
        self.copy(0, block).wait_recv()

    def begin(self):
        for way in (2, 0, 1):
            self.push(way, self.own)

    def drain(self):
        sent = self.buf.at[pl.ds(0, 2 * ZS - 1)]
        remote(sent, sent, self.send, self.recv.at[0], z=self.up).wait_send()


class Wide(Gather):
    def relay(self):
        self.arrive(self.other)
        for way in (0, 1):
            self.push(way, self.other)
        return [self.other]

    def blocks(self, d):
        out = []
        for col in (0, 1):
            for way in (0, 1):
                if d < 4 or way == col:
                    out.append((way, col, 2 * around(self.z, d if way else -d) + col))
        return out

    def step(self, d):
        for way, col, block in self.blocks(d):
            self.arrive(block)
            if d < 3 or (d == 3 and way == col):
                self.push(way, block)
        return [block for _, _, block in self.blocks(d)]

    def ready(self, n):
        return [block for _, _, block in self.blocks(n)] if n else [self.other]

    def phases(self):
        return [self.relay] + [functools.partial(self.step, d) for d in (1, 2, 3, 4)]


class Narrow(Gather):
    def begin(self):
        for way in (0, 1, 2):
            self.push(way, self.own)

    def blocks(self, d):
        if d == 4:
            return [(None, 2 * around(self.z, 4) + self.xl)]
        return [(way, 2 * around(self.z, d if way else -d) + self.xl) for way in (0, 1)]

    def crossed(self, d):
        places = [self.z] if d == 0 else [around(self.z, 4)] if d == 4 else [around(self.z, -d), around(self.z, d)]
        return [2 * place + 1 - self.xl for place in places]

    def step(self, d):
        out = []
        if d < 5:
            for way, block in self.blocks(d):
                self.arrive(block)
                if d < 3:
                    self.push(way, block)
                if d == 3:
                    pl.when(self.turn == way)(self.copy(way, block).start)
                self.push(2, block)
                out.append(block)
        for block in self.crossed(d - 1):
            self.arrive(block)
            out.append(block)
        return out

    def ready(self, n):
        return ([block for _, block in self.blocks(n + 1)] if n < 4 else []) + self.crossed(n)

    def phases(self):
        return [functools.partial(self.step, d) for d in (1, 2, 3, 4, 5)]


def needs(row, source, layers):
    half = layers // 2
    low = source < half
    wanted = (low & (row >= source)) | (jnp.logical_not(low) & (row <= layers - 1 - source))
    return wanted, jnp.where(low, source, source - (half - 1) + row)


def step_kernel(
    layers,
    res_ref,
    mlp_ref,
    enc_ref,
    enc_bias_ref,
    dec_ref,
    dec_bias_ref,
    err_ref,
    grad_ref,
    residual,
    mlp,
    encoder,
    enc_bias,
    weights,
    dec_bias,
    preact,
    codes,
    code_slots,
    rows_in,
    part,
    ring_out,
    ring_in,
    cross_out,
    cross_in,
    hand_out,
    hand_in,
    mirror_out,
    mirror_in,
    errors,
    sums,
    terms_out,
    terms_in,
    load_sem,
    res_send,
    res_recv,
    code_send,
    relay_send,
    code_recv,
    ring_send,
    ring_recv,
    cross_send,
    cross_recv,
    hand_send,
    hand_recv,
    mirror_send,
    mirror_recv,
    back_send,
    gather_send,
    gather_recv,
    term_send,
    term_recv,
):
    half = layers // 2
    me, z, xl = lax.axis_index("layer"), lax.axis_index("z"), lax.axis_index("xl")
    _, slots, tokens, feats = code_slots.shape
    width = part.shape[4]
    bf16, f32 = jnp.bfloat16, jnp.float32
    heavy = me < half
    own_slots = jnp.where(heavy, me + 1, half)
    mirror = layers - 1 - me
    turn = lax.rem(me, 2)
    up, down = around(z, 1), around(z, -1)
    mine = 2 * z + xl
    on_heavy = pl.when(heavy)
    on_light = pl.when(jnp.logical_not(heavy))

    loads = [
        pltpu.make_async_copy(res_ref.at[pl.ds(h * tokens, tokens)], residual.at[h, mine], load_sem.at[h]) for h in (0, 1)
    ]
    loads += [
        pltpu.make_async_copy(enc_ref, encoder, load_sem.at[2]),
        pltpu.make_async_copy(enc_bias_ref, enc_bias, load_sem.at[3]),
        pltpu.make_async_copy(dec_ref, weights, load_sem.at[4]),
        pltpu.make_async_copy(mlp_ref, mlp, load_sem.at[5]),
        pltpu.make_async_copy(dec_bias_ref, dec_bias, load_sem.at[6]),
    ]
    for load in loads:
        load.start()

    barrier = pltpu.get_barrier_semaphore()
    peers = [{"z": up}, {"z": down}, {"xl": 1 - xl}]
    peers += [{"layer": lax.rem(me + k, layers)} for k in range(1, layers)]
    for peer in peers:
        pl.semaphore_signal(barrier, inc=1, device_id=peer, device_id_type=MESH)
    pl.semaphore_wait(barrier, len(peers))

    drains = []

    def stream(h):
        wide = h == 0
        kind = Wide if wide else Narrow
        here = pl.ds(h * tokens, tokens)

        inputs = kind(residual.at[h], res_send.at[h], res_recv.at[h], z, xl, turn)
        loads[h].wait()
        inputs.begin()
        yield

        if wide:
            loads[2].wait()
            loads[3].wait()

        def encode(blocks):
            total = preact[h]
            for block in blocks:
                rows = pl.ds(pl.multiple_of(block * width, width), width)
                total = total + jnp.dot(residual[h, block], encoder[rows, :], preferred_element_type=f32)
            preact[h] = total

        preact[h] = jnp.zeros((tokens, feats), f32) + enc_bias[...]
        encode([inputs.own])
        for n, phase in enumerate(inputs.phases()):
            encode(phase())
            if n < 4:
                yield
        codes[h] = jnp.maximum(preact[h], 0.0).astype(bf16)

        def code_copy(k):
            chip = lax.rem(me // 2 + k, half)
            row = 2 * chip + jnp.where(heavy, 1, 0)
            wanted, slot = needs(row, me, layers)
            wanted = wanted & (row != me)
            slot = jnp.where(wanted, slot, 0)
            copy = remote(codes.at[h], code_slots.at[h, slot], code_send.at[h, k], code_recv.at[h, slot], layer=row)
            return wanted, copy

        def code_relay(n):
            source = n + half * (1 - turn)
            here, slot = needs(me, source, layers)
            here = here & (source != me)
            slot = jnp.where(here, slot, 0)
            partner = me + 1 - 2 * turn
            there, far = needs(partner, source, layers)
            there = here & there & (source != partner)
            far = jnp.where(there, far, 0)
            copy = remote(
                code_slots.at[h, slot], code_slots.at[h, far], relay_send.at[h, n], code_recv.at[h, far], layer=partner
            )
            return here, slot, there, copy

        def code_wait(slot):
            at = code_slots.at[h, slot]
            return remote(at, at, code_send.at[h, 0], code_recv.at[h, slot], layer=mirror).wait_recv

        for k in range(half):
            wanted, copy = code_copy(k)
            pl.when(wanted)(copy.start)

        @on_heavy
        def _():
            code_slots[h, me] = codes[h]

        @on_light
        def _():
            code_slots[h, slots - 1] = jnp.zeros((tokens, feats), bf16)

        yield
        for n in range(half):
            arrived, slot, there, copy = code_relay(n)
            pl.when(arrived)(code_wait(slot))
            pl.when(there)(copy.start)
        for n in range(half):
            source = n + half * turn
            arrived, slot = needs(me, source, layers)
            arrived = arrived & (source != me)
            pl.when(arrived)(code_wait(jnp.where(arrived, slot, 0)))
        for j in range(slots):
            cols = pl.ds(j * feats, feats)
            block = code_slots[h, j]
            own = j < own_slots
            rows_in[h, 0:tokens, cols] = jnp.where(own, block, jnp.zeros_like(block))
            rows_in[h, tokens:, cols] = jnp.where(own, jnp.zeros_like(block), block)
        if wide:
            for load in loads[4:]:
                load.wait()

        def decode(blocks):
            def columns(block):
                return weights[:, pl.ds(pl.multiple_of(block * width, width), width)]

            @on_heavy
            def _():
                for block in blocks:
                    both = jnp.dot(rows_in[h], columns(block), preferred_element_type=f32)
                    part[h, 0, block] = both[:tokens]
                    part[h, 1, block] = both[tokens:]

            @on_light
            def _():
                for block in blocks:
                    part[h, 0, block] = jnp.dot(rows_in[h, 0:tokens, :], columns(block), preferred_element_type=f32)

        def target(way, d):
            return around(z, jnp.where(way == 0, d, -d))

        def ring_copy(a, way, j, col):
            at = (h, a, way, j, col)
            return remote(
                ring_out.at[at], ring_in.at[at], ring_send.at[h, a], ring_recv.at[at], z=jnp.where(way == 0, up, down)
            )

        def cross_copy(a):
            return remote(cross_out.at[a], cross_in.at[a], cross_send.at[a], cross_recv.at[a], xl=1 - xl)

        def hand_copy(a, place):
            return remote(
                hand_out.at[a, place], hand_in.at[a, place], hand_send.at[a], hand_recv.at[a, place], xl=1 - xl
            )

        def ring_pieces(j):
            if wide:
                return [(way, col) for col in (0, 1) for way in (0, 1) if j > 0 or way == col]
            return [(turn, 0)] if j == 0 else [(turn, 0), (1 - turn, 0)]

        def block_of(way, d, col):
            return 2 * target(way, d) + (col if wide else xl)

        def hand_over(steps):
            places = [around(z, s) for s in steps]
            decode([2 * place + 1 - xl for place in places])

            def send(a):
                for place in places:
                    hand_out[a, place] = part[h, a, 2 * place + 1 - xl].astype(bf16)
                    hand_copy(a, place).start()

            on_heavy(lambda: send(1))
            send(0)

        def ring_decode(j):
            decode([block_of(way, 4 - j, col) for way, col in ring_pieces(j)])

        def ring_step(a, j):
            before = ring_pieces(j - 1) if j else []
            for n, (way, col) in enumerate(ring_pieces(j)):
                place = target(way, 4 - j)
                value = part[h, a, block_of(way, 4 - j, col)]
                if not wide:
                    hand_copy(a, place).wait_recv()
                    value = value + hand_in[a, place].astype(f32)
                if (way, col) in before if wide else n < len(before):
                    ring_copy(a, way, j - 1, col).wait_recv()
                    value = value + ring_in[h, a, way, j - 1, col].astype(f32)
                ring_out[h, a, way, j, col] = value.astype(bf16)
                ring_copy(a, way, j, col).start()

        def ring_end(a):
            for col in (0, 1) if wide else (0,):
                for way in (0, 1):
                    ring_copy(a, way, 3, col).wait_recv()

            def total(block, col):
                both = ring_in[h, a, 0, 3, col].astype(f32) + ring_in[h, a, 1, 3, col].astype(f32)
                return part[h, a, block] + both

            if wide:
                cross_out[a] = total(2 * z + 1 - xl, 1 - xl).astype(bf16)
                cross_copy(a).start()
                part[h, a, mine] = total(mine, xl)
            else:
                hand_copy(a, z).wait_recv()
                part[h, a, mine] = total(mine, 0) + hand_in[a, z].astype(f32)

        def ring_sum(a):
            if wide:
                cross_copy(a).wait_recv()
                return part[h, a, mine] + cross_in[a].astype(f32)
            return part[h, a, mine]

        def mirror_copy():
            return remote(mirror_out.at[h], mirror_in.at[h], mirror_send.at[h], mirror_recv.at[h], layer=mirror)

        if not wide:
            hand_over((4, 3, -3))
            yield
            hand_over((2, -2, 1, -1, 0))
        for j in range(4):
            ring_decode(j)
            on_heavy(lambda: ring_step(1, j))
            ring_step(0, j)
            yield
        decode([mine, 2 * z + 1 - xl] if wide else [mine])
        on_heavy(lambda: ring_end(1))
        ring_end(0)
        yield

        @on_heavy
        def _():
            mirror_out[h] = ring_sum(1).astype(bf16)
            mirror_copy().start()

        yield
        bias = dec_bias[:, pl.ds(pl.multiple_of(mine * width, width), width)]
        part[h, 0, mine] = ring_sum(0) + bias - mlp[here, :].astype(f32)

        @on_light
        def _():
            mirror_copy().wait_recv()
            part[h, 0, mine] = part[h, 0, mine] + mirror_in[h].astype(f32)

        error = part[h, 0, mine].astype(bf16)
        err_ref[here, :] = error
        errors[h, 0, mine] = error

        first, second = [
            kind(errors.at[h, a], gather_send.at[h, a], gather_recv.at[h, a], z, xl, turn) for a in (0, 1)
        ]

        def back_copy():
            return remote(
                errors.at[h, 0, mine], errors.at[h, 1, mine], back_send.at[h], gather_recv.at[h, 1, mine], layer=mirror
            )

        on_light(lambda: back_copy().start())
        first.begin()
        yield
        def term_copy(j):
            source = jnp.where(j < own_slots, j, j + (half - 1) - me)
            return source, remote(
                terms_out.at[h, j], terms_in.at[h, me], term_send.at[h], term_recv.at[h, me], layer=source
            )

        def backward(a, blocks, start, end):
            def one(j, carry):
                rows = pl.ds(pl.multiple_of(j * feats, feats), feats)
                total = jnp.zeros((tokens, feats), f32) if start else sums[h, j]
                for block in blocks:
                    cols = pl.ds(pl.multiple_of(block * width, width), width)
                    total = total + lax.dot_general(
                        errors[h, a, block],
                        weights[rows, cols],
                        (((1,), (1,)), ((), ())),
                        preferred_element_type=f32,
                    )
                if not end:
                    sums[h, j] = total
                    return carry
                source, copy = term_copy(j)

                @pl.when(source == me)
                def _():
                    grad_ref[here, :] = total

                @pl.when(source != me)
                def _():
                    terms_out[h, j] = total.astype(bf16)
                    copy.start()

                return carry

            lax.fori_loop(own_slots if a else 0, slots if a else own_slots, one, 0)

        grad_ref[here, :] = jnp.zeros((tokens, feats), f32)
        early, late = first.phases(), second.phases()
        for phase in early[:2]:
            phase()
            yield

        @on_heavy
        def _():
            back_copy().wait_recv()
            second.begin()

        yield
        early[2]()
        yield

        @on_heavy
        def _():
            late[0]()

        yield
        early[3]()
        yield

        @on_heavy
        def _():
            late[1]()
            backward(1, [second.own] + second.ready(0) + second.ready(1), True, False)

        yield
        early[4]()
        yield

        @on_heavy
        def _():
            late[2]()

        yield
        backward(0, list(range(2 * ZS)), True, True)
        yield

        @on_heavy
        def _():
            late[3]()
            backward(1, second.ready(2) + second.ready(3), False, False)

        yield

        @on_heavy
        def _():
            backward(1, late[4](), False, True)

        yield

        def collect(row, carry):
            wanted, _ = needs(row, me, layers)

            @pl.when(wanted & (row != me))
            def _():
                remote(
                    terms_out.at[h, 0], terms_in.at[h, row], term_send.at[h], term_recv.at[h, row], layer=mirror
                ).wait_recv()
                grad_ref[here, :] += terms_in[h, row].astype(f32)

            return carry

        lax.fori_loop(0, layers, collect, 0)

        def drain():
            inputs.drain()
            for k in range(half):
                wanted, copy = code_copy(k)
                pl.when(wanted)(copy.wait_send)
                _, _, there, copy = code_relay(k)
                pl.when(there)(copy.wait_send)

            def drain_sums(a):
                sent = residual.at[h, pl.ds(0, 14 if wide else 7)]
                remote(sent, sent, ring_send.at[h, a], ring_recv.at[h, a, 0, 0, 0], z=up).wait_send()
                if wide:
                    cross_copy(a).wait_send()
                else:
                    sent = hand_out.at[a]
                    remote(sent, sent, hand_send.at[a], hand_recv.at[a, 0], xl=1 - xl).wait_send()

            drain_sums(0)
            first.drain()
            on_light(lambda: back_copy().wait_send())

            @on_heavy
            def _():
                drain_sums(1)
                mirror_copy().wait_send()
                second.drain()

            sent = terms_out.at[h, pl.ds(0, half)]
            remote(sent, sent, term_send.at[h], term_recv.at[h, 0], layer=mirror).wait_send()

        drains.append(drain)

    running = {"A": stream(0), "B": stream(1)}
    for name in ORDER + 40 * "AB":
        if name in running and next(running[name], "end") == "end":
            del running[name]
    for drain in drains:
        drain()


def shards(residual_in, mlp_out, encoder, encoder_bias, decoder, decoder_bias):
    layers = lax.axis_size("layer")
    tokens, width = residual_in.shape[1:]
    feats = encoder.shape[2]
    slots = decoder.shape[1]
    depth = decoder.shape[3]
    blocks = 2 * ZS
    part = tokens // 2
    bf16, f32 = jnp.bfloat16, jnp.float32
    dma, vmem = pltpu.SemaphoreType.DMA, pltpu.VMEM

    error, grad = pl.pallas_call(
        functools.partial(step_kernel, layers),
        out_shape=(
            vmem((tokens, width), bf16),
            vmem((tokens, feats), f32),
        ),
        in_specs=[pl.BlockSpec(memory_space=pltpu.HBM)] * 6,
        out_specs=(pl.BlockSpec(memory_space=vmem),) * 2,
        scratch_shapes=[
            vmem((2, blocks, part, width), bf16),
            vmem((tokens, width), bf16),
            vmem((depth, feats), bf16),
            vmem((1, feats), f32),
            vmem((slots * feats, depth), bf16),
            vmem((1, depth), f32),
            vmem((2, part, feats), f32),
            vmem((2, part, feats), bf16),
            vmem((2, slots, part, feats), bf16),
            vmem((2, tokens, slots * feats), bf16),
            vmem((2, 2, blocks, part, width), f32),
            vmem((2, 2, 2, 4, 2, part, width), bf16),
            vmem((2, 2, 2, 4, 2, part, width), bf16),
            vmem((2, part, width), bf16),
            vmem((2, part, width), bf16),
            vmem((2, ZS, part, width), bf16),
            vmem((2, ZS, part, width), bf16),
            vmem((2, part, width), bf16),
            vmem((2, part, width), bf16),
            vmem((2, 2, blocks, part, width), bf16),
            vmem((2, slots, part, feats), f32),
            vmem((2, slots, part, feats), bf16),
            vmem((2, layers, part, feats), bf16),
            dma((7,)),
            dma((2,)),
            dma((2, blocks)),
            dma((2, layers // 2)),
            dma((2, layers // 2)),
            dma((2, slots)),
            dma((2, 2)),
            dma((2, 2, 2, 4, 2)),
            dma((2,)),
            dma((2,)),
            dma((2,)),
            dma((2, ZS)),
            dma((2,)),
            dma((2,)),
            dma((2,)),
            dma((2, 2)),
            dma((2, 2, blocks)),
            dma((2,)),
            dma((2, layers)),
        ],
        compiler_params=pltpu.CompilerParams(
            collective_id=0, has_side_effects=True, vmem_limit_bytes=60 << 20
        ),
        name="transcoder_step",
    )(residual_in[0], mlp_out[0], encoder[0], encoder_bias, decoder[0].reshape(slots * feats, depth), decoder_bias)
    return error[None], grad[None]


def solution(mesh):
    split = Mesh(mesh.devices.reshape(mesh.shape["layer"], ZS, 2), ("layer", "z", "xl"))
    placed = (
        P("layer", None, FEAT),
        P("layer", None, FEAT),
        P("layer", None, FEAT),
        P("layer", FEAT),
        P("layer", None, FEAT, None),
        P("layer", None),
    )
    return jax.shard_map(
        shards,
        mesh=split,
        in_specs=placed,
        out_specs=(P("layer", None, FEAT), P("layer", None, FEAT)),
        check_vma=False,
    )
```
